32 devices in a mesh: dp: 1 (over z), ep: 32 (over y, x, core).
Axes of the slice: x: 4, y: 4, z: 1, core: 2. Of those that a mesh axis runs over, the one named last changes fastest.
The devices are a block of a 4x4x8 slice.
Arguments:
- resid_in: bfloat16 [2, 32, 1024, 1024], P(None, ('dp', 'ep'))
- expert_idx: int32 [2, 32, 1024, 8], P(None, ('dp', 'ep'))
- expert_slot: int32 [2, 32, 1024, 8], P(None, ('dp', 'ep'))
- w_query: bfloat16 [1024, 16, 64], replicated
- w_key: bfloat16 [1024, 8, 64], replicated
- w_value: bfloat16 [1024, 8, 64], replicated
- w_out: bfloat16 [16, 64, 1024], replicated
- w_gate: bfloat16 [1024, 4096], replicated
- w_up: bfloat16 [1024, 4096], replicated
- w_down: bfloat16 [4096, 1024], replicated
- w_router: bfloat16 [1024, 32], replicated
- norm_attn: bfloat16 [1024], replicated
- norm_ffn: bfloat16 [1024], replicated
- norm_moe: bfloat16 [1024], replicated
- expert_gate: bfloat16 [32, 1024, 512], P('ep')
- expert_up: bfloat16 [32, 1024, 512], P('ep')
- expert_down: bfloat16 [32, 512, 1024], P('ep')
Outputs:
- output: bfloat16 [2, 32, 1024, 1024], P(None, ('dp', 'ep'))
All inputs are finite; a program needn't handle non-finite values.
Results may differ from the reference program's by a relative error of at most 0.010065.
Values are sent between devices in bfloat16 or wider.
A program may use at most 768 MiB of HBM per device.

```python
import jax
import jax.numpy as jnp
from jax import lax

D = 1024
HEADS = 16
KV_HEADS = 8
HEAD = 64
EXPERTS = 32
TOP = 8
FE = 512
FF = 4096
SEQ = 1024
SEQS = 1
GROUP = 32

TOK_MB = SEQS * SEQ
CAP = 2 * TOK_MB * TOP // EXPERTS
EPS = 1e-6
ROPE_BASE = 10000.0


def draw_device(rng_key):
    count_key, label_key, order_key = jax.random.split(rng_key, 3)
    pair_left = jax.random.randint(count_key, (EXPERTS // 2,), 0, CAP + 1)
    pair_left = pair_left.at[0].set(CAP)
    counts = jnp.stack([pair_left, CAP - pair_left], axis=1).reshape(EXPERTS)
    count_ends = jnp.cumsum(counts)
    count_starts = count_ends - counts
    copy_pos = jnp.arange(TOK_MB * TOP)
    sorted_ids = jnp.sum(copy_pos[:, None] >= count_ends[None, :], axis=1)
    slot_ranks = copy_pos - count_starts[sorted_ids]
    labels = jax.random.permutation(label_key, EXPERTS)[sorted_ids]
    token_order = jax.random.permutation(order_key, TOK_MB)
    ids_out = labels.reshape(TOP, TOK_MB).T[token_order]
    slots_out = slot_ranks.reshape(TOP, TOK_MB).T[token_order]
    return ids_out.astype(jnp.int32), slots_out.astype(jnp.int32)


def draw_routing(rng_key):
    device_keys = jax.random.split(rng_key, 2 * GROUP)
    ids_all, slots_all = jax.vmap(draw_device)(device_keys)
    return (ids_all.reshape(2, GROUP * SEQS, SEQ, TOP), slots_all.reshape(2, GROUP * SEQS, SEQ, TOP))


def setup_inputs(seed: int = 0, part: int = 0) -> dict:
    root_key = jax.random.key(seed)
    weight_keys = jax.random.split(root_key, 14)
    part_key = jax.random.fold_in(jax.random.key(seed + 1), part)
    act_key, route_key = jax.random.split(part_key)

    def normal_weight(rng_key, shape, fan_in, gain):
        raw_draw = jax.random.normal(rng_key, shape, jnp.float32)
        return (raw_draw * (gain * fan_in ** -0.5)).astype(jnp.bfloat16)

    def norm_scale(rng_key):
        return (1.0 + 0.3 * jax.random.normal(rng_key, (D,), jnp.float32)).astype(jnp.bfloat16)

    resid_in = jax.random.normal(act_key, (2, GROUP * SEQS, SEQ, D), jnp.float32).astype(jnp.bfloat16)
    expert_idx, expert_slot = draw_routing(route_key)
    return {
        'resid_in': resid_in,
        'expert_idx': expert_idx,
        'expert_slot': expert_slot,
        'w_query': normal_weight(weight_keys[0], (D, HEADS, HEAD), D, 2.0),
        'w_key': normal_weight(weight_keys[1], (D, KV_HEADS, HEAD), D, 1.0),
        'w_value': normal_weight(weight_keys[2], (D, KV_HEADS, HEAD), D, 1.0),
        'w_out': normal_weight(weight_keys[3], (HEADS, HEAD, D), HEADS * HEAD, 2.0),
        'w_gate': normal_weight(weight_keys[4], (D, FF), D, 1.0),
        'w_up': normal_weight(weight_keys[5], (D, FF), D, 1.0),
        'w_down': normal_weight(weight_keys[6], (FF, D), FF, 1.0),
        'w_router': normal_weight(weight_keys[7], (D, EXPERTS), D, 2.0),
        'norm_attn': norm_scale(weight_keys[8]),
        'norm_ffn': norm_scale(weight_keys[9]),
        'norm_moe': norm_scale(weight_keys[10]),
        'expert_gate': normal_weight(weight_keys[11], (EXPERTS, D, FE), D, 1.0),
        'expert_up': normal_weight(weight_keys[12], (EXPERTS, D, FE), D, 1.0),
        'expert_down': normal_weight(weight_keys[13], (EXPERTS, FE, D), FE, 2.0),
    }


def rms_norm(values, scale):
    widened = values.astype(jnp.float32)
    mean_sq = jnp.mean(widened * widened, axis=-1, keepdims=True)
    return (widened * lax.rsqrt(mean_sq + EPS) * scale.astype(jnp.float32)).astype(jnp.bfloat16)


def rotary(values):
    half_dim = HEAD // 2
    freqs = ROPE_BASE ** (-jnp.arange(half_dim, dtype=jnp.float32) * 2.0 / HEAD)
    angles = jnp.arange(SEQ, dtype=jnp.float32)[:, None] * freqs[None, :]
    cosine = jnp.cos(angles)[:, None, :]
    sine = jnp.sin(angles)[:, None, :]
    first = values[..., :half_dim]
    second = values[..., half_dim:]
    return jnp.concatenate([first * cosine - second * sine, second * cosine + first * sine], axis=-1)


def swiglu(normed, w_gate, w_up, w_down):
    gate_act = jnp.dot(normed, w_gate, preferred_element_type=jnp.float32)
    up_act = jnp.dot(normed, w_up, preferred_element_type=jnp.float32)
    hidden = (jax.nn.silu(gate_act) * up_act).astype(jnp.bfloat16)
    return jnp.dot(hidden, w_down, preferred_element_type=jnp.float32)


def reference(resid_in, expert_idx, expert_slot, w_query, w_key, w_value, w_out, w_gate, w_up, w_down, w_router, norm_attn, norm_ffn, norm_moe, expert_gate, expert_up, expert_down):
    group_heads = HEADS // KV_HEADS
    causal = jnp.arange(SEQ)[:, None] >= jnp.arange(SEQ)[None, :]
    query_flat = w_query.reshape(D, HEADS * HEAD)
    key_flat = w_key.reshape(D, KV_HEADS * HEAD)
    value_flat = w_value.reshape(D, KV_HEADS * HEAD)
    out_flat = w_out.reshape(HEADS * HEAD, D)

    def dense_sequence(resid):
        normed = rms_norm(resid, norm_attn)
        queries = rotary(jnp.dot(normed, query_flat, preferred_element_type=jnp.float32).reshape(SEQ, HEADS, HEAD)).astype(jnp.bfloat16)
        keys_rot = rotary(jnp.dot(normed, key_flat, preferred_element_type=jnp.float32).reshape(SEQ, KV_HEADS, HEAD)).astype(jnp.bfloat16)
        values_in = jnp.dot(normed, value_flat, preferred_element_type=jnp.float32).astype(jnp.bfloat16).reshape(SEQ, KV_HEADS, HEAD)
        keys_rep = jnp.repeat(keys_rot, group_heads, axis=1)
        values_rep = jnp.repeat(values_in, group_heads, axis=1)
        scores = jnp.einsum('qhe,khe->hqk', queries.astype(jnp.float32), keys_rep.astype(jnp.float32)) * (HEAD ** -0.5)
        probs = jax.nn.softmax(jnp.where(causal[None], scores, -1e30), axis=-1).astype(jnp.bfloat16)
        attended = jnp.einsum('hqk,khe->qhe', probs.astype(jnp.float32), values_rep.astype(jnp.float32)).astype(jnp.bfloat16)
        attn_out = jnp.dot(attended.reshape(SEQ, HEADS * HEAD), out_flat, preferred_element_type=jnp.float32)
        after_attn = (resid.astype(jnp.float32) + attn_out).astype(jnp.bfloat16)
        ffn_out = swiglu(rms_norm(after_attn, norm_ffn), w_gate, w_up, w_down)
        return after_attn.astype(jnp.float32) + ffn_out

    token_count = 2 * GROUP * TOK_MB
    dense_out = lax.map(dense_sequence, resid_in.reshape(2 * GROUP * SEQS, SEQ, D)).reshape(token_count, D)

    normed_moe = rms_norm(resid_in.reshape(token_count, D), norm_moe)
    logits = jnp.dot(normed_moe, w_router, preferred_element_type=jnp.float32)
    route_ids = expert_idx.reshape(token_count, TOP)
    route_slots = expert_slot.reshape(token_count, TOP)
    gates = jax.nn.softmax(jnp.take_along_axis(logits, route_ids, axis=1), axis=-1)
    token_pos = jnp.arange(token_count, dtype=jnp.int32)
    micro_of = token_pos // (GROUP * TOK_MB)
    device_of = (token_pos // TOK_MB) % GROUP
    buf_pos = ((route_ids * 2 + micro_of[:, None]) * GROUP + device_of[:, None]) * CAP + route_slots
    copy_count = token_count * TOP
    copy_of_row = jnp.full((EXPERTS * 2 * GROUP * CAP,), copy_count, jnp.int32)
    copy_of_row = copy_of_row.at[buf_pos.reshape(-1)].set(jnp.arange(copy_count, dtype=jnp.int32))
    copy_of_row = copy_of_row.reshape(EXPERTS, 2 * GROUP * CAP)
    gate_flat = gates.reshape(copy_count)

    def expert_step(accum_out, expert_args):
        w_a, w_b, w_c, row_copies = expert_args
        row_tokens = row_copies // TOP
        rows_in = jnp.take(normed_moe, row_tokens, axis=0, mode='fill', fill_value=0)
        expert_out = swiglu(rows_in, w_a, w_b, w_c).astype(jnp.bfloat16)
        row_gates = jnp.take(gate_flat, row_copies, mode='fill', fill_value=0)
        accum_out = accum_out.at[row_tokens].add(row_gates[:, None] * expert_out.astype(jnp.float32), mode='drop')
        return accum_out, None

    moe_out = lax.scan(expert_step, jnp.zeros((token_count, D), jnp.float32), (expert_gate, expert_up, expert_down, copy_of_row))[0]
    return (dense_out + moe_out).astype(jnp.bfloat16).reshape(2, GROUP * SEQS, SEQ, D)
```

```python
import functools

import jax
import jax.numpy as jnp
from jax import lax
from jax.experimental import pallas as pl
from jax.experimental.pallas import tpu as pltpu
from jax.sharding import PartitionSpec as P

EPS = 1e-6
ROPE_BASE = 10000.0


def rms_norm(values, scale):
    widened = values.astype(jnp.float32)
    mean_sq = jnp.mean(widened * widened, axis=-1, keepdims=True)
    return (widened * lax.rsqrt(mean_sq + EPS) * scale.astype(jnp.float32)).astype(jnp.bfloat16)


def rotary(values):
    seq_len = values.shape[-3]
    head_dim = values.shape[-1]
    half_dim = head_dim // 2
    freqs = ROPE_BASE ** (-jnp.arange(half_dim, dtype=jnp.float32) * 2.0 / head_dim)
    angles = jnp.arange(seq_len, dtype=jnp.float32)[:, None] * freqs[None, :]
    cosine = jnp.cos(angles)[:, None, :]
    sine = jnp.sin(angles)[:, None, :]
    first = values[..., :half_dim]
    second = values[..., half_dim:]
    return jnp.concatenate([first * cosine - second * sine, second * cosine + first * sine], axis=-1)


def dense_branch(resid, norm_attn, w_query, w_key, w_value, w_out, norm_ffn, w_gate, w_up, w_down):
    batch, seq_len = resid.shape[0], resid.shape[1]
    heads, head_dim = w_query.shape[1], w_query.shape[2]
    kv_heads = w_key.shape[1]
    normed = rms_norm(resid, norm_attn)
    queries = rotary(jnp.einsum('bsd,dhe->bshe', normed, w_query, preferred_element_type=jnp.float32)).astype(jnp.bfloat16)
    keys_rot = rotary(jnp.einsum('bsd,dhe->bshe', normed, w_key, preferred_element_type=jnp.float32)).astype(jnp.bfloat16)
    values_in = jnp.einsum('bsd,dhe->bshe', normed, w_value, preferred_element_type=jnp.float32).astype(jnp.bfloat16)
    grouped = queries.reshape(batch, seq_len, kv_heads, heads // kv_heads, head_dim)
    scores = jnp.einsum('bqgre,bkge->bgrqk', grouped, keys_rot, preferred_element_type=jnp.float32) * (head_dim ** -0.5)
    causal = jnp.arange(seq_len)[:, None] >= jnp.arange(seq_len)[None, :]
    probs = jax.nn.softmax(jnp.where(causal, scores, -1e30), axis=-1).astype(jnp.bfloat16)
    attended = jnp.einsum('bgrqk,bkge->bqgre', probs, values_in, preferred_element_type=jnp.float32).astype(jnp.bfloat16)
    attn_out = jnp.einsum('bshe,hed->bsd', attended.reshape(batch, seq_len, heads, head_dim), w_out, preferred_element_type=jnp.float32)
    after_attn = (resid.astype(jnp.float32) + attn_out).astype(jnp.bfloat16)
    normed_ffn = rms_norm(after_attn, norm_ffn)
    gate_act = jnp.einsum('bsd,df->bsf', normed_ffn, w_gate, preferred_element_type=jnp.float32)
    up_act = jnp.einsum('bsd,df->bsf', normed_ffn, w_up, preferred_element_type=jnp.float32)
    hidden = (jax.nn.silu(gate_act) * up_act).astype(jnp.bfloat16)
    down_act = jnp.einsum('bsf,fd->bsd', hidden, w_down, preferred_element_type=jnp.float32)
    return after_attn.astype(jnp.float32) + down_act


def route(normed, w_router, route_ids):
    logits = jnp.dot(normed, w_router, preferred_element_type=jnp.float32)
    experts = w_router.shape[1]
    picked = jnp.any(route_ids[:, :, None] == jnp.arange(experts, dtype=jnp.int32)[None, None, :], axis=1)
    top = jnp.max(jnp.where(picked, logits, -jnp.inf), axis=-1, keepdims=True)
    powers = jnp.where(picked, jnp.exp(jnp.where(picked, logits, top) - top), 0.0)
    return powers / jnp.sum(powers, axis=-1, keepdims=True)


def moe_kernel(row_tile, width, hidden, x_ref, gates_ref, base_ref, pack_ref, out_ref, total_ref):
    expert = pl.program_id(0)
    rows = x_ref.shape[0]

    @pl.when(expert == 0)
    def _():
        total_ref[...] = base_ref[...]

    lanes = lax.broadcasted_iota(jnp.int32, (row_tile, gates_ref.shape[1]), 1)

    def tile_step(tile, carry):
        part = pl.ds(pl.multiple_of(tile * row_tile, row_tile), row_tile)
        tokens = x_ref[part, :]
        weight = jnp.sum(jnp.where(lanes == expert, gates_ref[part, :], 0.0), axis=1, keepdims=True)
        gate_act = jnp.dot(tokens, pack_ref[0, :width, :], preferred_element_type=jnp.float32)
        up_act = jnp.dot(tokens, pack_ref[0, width:2 * width, :], preferred_element_type=jnp.float32)
        mixed = (jax.nn.silu(gate_act) * up_act).astype(jnp.bfloat16)
        for side in range(2):
            cols = pl.ds(side * (width // 2), width // 2)
            start = 2 * width + side * hidden
            down = jnp.dot(mixed, pack_ref[0, start:start + hidden, :], preferred_element_type=jnp.float32)
            down = down.astype(jnp.bfloat16).astype(jnp.float32)
            total_ref[part, cols] += jnp.where(weight > 0.0, weight * down, 0.0)
        return carry

    lax.fori_loop(0, rows // row_tile, tile_step, 0)

    @pl.when(expert == pl.num_programs(0) - 1)
    def _():
        out_ref[...] = total_ref[...].astype(out_ref.dtype)


def moe_all(tokens, gates, base, packed):
    rows, width = tokens.shape
    experts, pack_rows, hidden = packed.shape
    row_tile = 512
    once = pl.Buffered(buffer_count=1)
    return pl.pallas_call(
        functools.partial(moe_kernel, row_tile, width, hidden),
        out_shape=jax.ShapeDtypeStruct((rows, width), jnp.bfloat16),
        grid=(experts,),
        in_specs=[
            pl.BlockSpec((rows, width), lambda e: (0, 0), pipeline_mode=once),
            pl.BlockSpec((rows, gates.shape[1]), lambda e: (0, 0), pipeline_mode=once),
            pl.BlockSpec((rows, width), lambda e: (0, 0), pipeline_mode=once),
            pl.BlockSpec((1, pack_rows, hidden), lambda e: (e, 0, 0)),
        ],
        out_specs=pl.BlockSpec((rows, width), lambda e: (0, 0), pipeline_mode=once),
        scratch_shapes=[pltpu.VMEM((rows, width), jnp.float32)],
        compiler_params=pltpu.CompilerParams(dimension_semantics=("arbitrary",), vmem_limit_bytes=60 * 1024 * 1024),
        cost_estimate=pl.CostEstimate(flops=rows * experts * 6 * width * hidden, bytes_accessed=packed.size * 2, transcendentals=0),
    )(tokens, gates, base, packed)


def solution(mesh):
    tok_spec = P(None, ('dp', 'ep'), None, None)
    rep_one = P(None)
    rep_two = P(None, None)
    rep_three = P(None, None, None)
    expert_spec = P('ep', None, None)

    def local_program(resid_in, expert_idx, expert_slot, w_query, w_key, w_value, w_out, w_gate, w_up, w_down, w_router, norm_attn, norm_ffn, norm_moe, expert_gate, expert_up, expert_down):
        micro_count, seqs, seq_len, width = resid_in.shape
        choices = expert_idx.shape[-1]
        rows = micro_count * seqs * seq_len
        half = width // 2
        packed = jnp.concatenate([expert_gate, expert_up, expert_down[:, :, :half], expert_down[:, :, half:]], axis=1)
        packed = lax.all_gather(packed, 'ep', axis=0, tiled=True)
        resid = resid_in.reshape(micro_count * seqs, seq_len, width)
        tokens = rms_norm(resid.reshape(rows, width), norm_moe)
        gates = route(tokens, w_router, expert_idx.reshape(rows, choices))
        dense_out = dense_branch(resid, norm_attn, w_query, w_key, w_value, w_out, norm_ffn, w_gate, w_up, w_down)
        out = moe_all(tokens, gates, dense_out.reshape(rows, width), packed)
        return out.reshape(resid_in.shape)

    return jax.shard_map(local_program, mesh=mesh, in_specs=(tok_spec, tok_spec, tok_spec, rep_three, rep_three, rep_three, rep_three, rep_two, rep_two, rep_two, rep_two, rep_one, rep_one, rep_one, expert_spec, expert_spec, expert_spec), out_specs=tok_spec, check_vma=False)
```

```python
import functools
import math

import jax
import jax.numpy as jnp
import numpy as np
from jax import lax
from jax.experimental import pallas as pl
from jax.experimental.pallas import tpu as pltpu
from jax.sharding import PartitionSpec as P

EPS = 1e-6
ROPE_BASE = 10000.0
LANES = 128
F32 = jnp.float32
BF16 = jnp.bfloat16

BLOCKS = ((0, 0), (1, 0), (3, 0), (0, 1), (0, 3), (1, 1), (1, 3), (3, 1), (3, 3), (2, 0), (0, 2), (2, 1), (1, 2), (2, 3), (3, 2), (2, 2))
SIDE = 4
STEPS = ((1, 0), (-1, 0), (0, 1), (0, -1))
GATE, UP, LOW, HIGH = 0, 1, 2, 3


def block_of(dx, dy):
    return BLOCKS.index((dx % SIDE, dy % SIDE))


def send_plan():
    plan = [[], [], [], [], []]
    used = [0, 0, 0, 0]

    def send(service, link, pieces, dx, dy):
        sx, sy = STEPS[link]
        for piece in pieces:
            plan[service].append((link, used[link], piece, block_of(dx, dy), block_of(dx + sx, dy + sy)))
            used[link] += 1

    send(0, 0, (GATE, LOW, UP, HIGH), 0, 0)
    send(0, 1, (LOW, GATE, HIGH, UP), 0, 0)
    send(0, 2, (UP, HIGH, GATE, LOW), 0, 0)
    send(0, 3, (HIGH, UP, LOW, GATE), 0, 0)

    low_first, gate_first, up_first, high_first = (LOW, GATE), (GATE, LOW), (UP, HIGH), (HIGH, UP)
    for link, piece, near in ((0, GATE, (1, 0)), (1, LOW, (3, 0)), (2, UP, (0, 1)), (3, HIGH, (0, 3))):
        send(1, link, (piece,), *near)
    for near in (1, 3):
        for link, pieces in enumerate((up_first, high_first)):
            send(1, link, pieces, 0, near)
        for link, pieces in enumerate((gate_first, low_first)):
            send(1, 2 + link, pieces, near, 0)

    for link, piece, near in ((0, HIGH, (1, 0)), (1, UP, (3, 0)), (2, LOW, (0, 1)), (3, GATE, (0, 3))):
        send(2, link, (piece,), *near)
    for link, pieces in enumerate((up_first, high_first)):
        send(2, link, pieces, 0, 2)
    for link, pieces in enumerate((gate_first, low_first)):
        send(2, 2 + link, pieces, 2, 0)

    for near in (1, 3):
        for link, piece, far in ((0, UP, (1, near)), (1, HIGH, (3, near)), (2, GATE, (near, 1)), (3, LOW, (near, 3))):
            send(3, link, (piece,), *far)

    for link, piece, near in ((0, HIGH, (1, 2)), (1, UP, (3, 2)), (2, LOW, (2, 1)), (3, GATE, (2, 3))):
        send(4, link, (piece,), *near)
    return plan


def wait_plan():
    both, first, second = (GATE, LOW, UP, HIGH), (GATE, LOW), (UP, HIGH)
    waits = [
        [],
        [((1, 0), first), ((3, 0), first), ((0, 1), second), ((0, 3), second)],
        [((1, 0), second), ((3, 0), second), ((0, 1), first), ((0, 3), first), ((2, 0), first), ((0, 2), second)],
        [((1, 1), both), ((1, 3), both), ((3, 1), both), ((3, 3), both)],
        [((2, 0), second), ((0, 2), first), ((2, 1), first), ((2, 3), first), ((1, 2), second), ((3, 2), second)],
        [((1, 2), first), ((3, 2), first), ((2, 1), second), ((2, 3), second), ((2, 2), both)],
    ]
    done = [
        [(0, 0)],
        [],
        [(1, 0), (3, 0), (0, 1), (0, 3)],
        [(1, 1), (1, 3), (3, 1), (3, 3)],
        [(2, 0), (0, 2)],
        [(2, 1), (1, 2), (2, 3), (3, 2), (2, 2)],
    ]
    return waits, done


def matmul(left, right):
    return jnp.dot(left, right, preferred_element_type=F32)


def matmul_t(left, right):
    return lax.dot_general(left, right, (((1,), (1,)), ((), ())), preferred_element_type=F32)


def norm_scale_of(values):
    return lax.rsqrt(jnp.mean(values * values, axis=-1, keepdims=True) + EPS)


def fused_kernel(
    dims,
    x_hbm, ids_hbm, router_hbm, norms_hbm, rope_hbm, wq_hbm, wk_hbm, wv_hbm, wo_hbm, fg_hbm, fu_hbm, fd_hbm, eg_hbm, eu_hbm, ed_hbm,
    out_hbm, gg_hbm, gu_hbm, gd_hbm,
    xs, acc, gates, qs, ks, vs, os, s_outer, s_inner, p_outer, p_inner, tops, sums, ids, router, norms, rope, wqkv, wo, wg, wu, wd,
    load_sem, w_sem, out_sem, ici_send, ici_recv, d2d_send, d2d_recv,
):
    rows, width, seq, hidden, heads, kv_heads, head = dims
    micro = rows // seq
    half = hidden // 2
    experts = 2 * len(BLOCKS)
    ffn_steps = fg_hbm.shape[1] // hidden
    steps = ffn_steps + experts
    me = lax.axis_index('ep')
    core = lax.rem(me, 2)
    col = lax.rem(me // 2, SIDE)
    row = me // (2 * SIDE)

    def device(dx, dy, flip):
        cx = lax.rem(col + dx + SIDE, SIDE)
        cy = lax.rem(row + dy + SIDE, SIDE)
        return {'ep': (cy * SIDE + cx) * 2 + lax.rem(core + flip, 2)}

    def piece_ref(block, piece):
        if block == 0:
            return (eg_hbm.at[0], eu_hbm.at[0], ed_hbm.at[0, pl.ds(0, half)], ed_hbm.at[0, pl.ds(half, half)])[piece]
        return slot_ref(2 * block, piece)

    def slot_ref(slot, piece):
        return (gg_hbm.at[slot], gu_hbm.at[slot], gd_hbm.at[slot, pl.ds(0, half)], gd_hbm.at[slot, pl.ds(half, half)])[piece]

    def ici_copy(link, place, piece, source, target):
        return pltpu.make_async_remote_copy(
            src_ref=piece_ref(source, piece), dst_ref=slot_ref(2 * target, piece),
            send_sem=ici_send.at[link, place], recv_sem=ici_recv.at[target, piece],
            device_id=device(*STEPS[link], 0), device_id_type=pl.DeviceIdType.MESH)

    def d2d_copies(block, own):
        sources = (eg_hbm.at[0], eu_hbm.at[0], ed_hbm.at[0]) if own else (gg_hbm.at[2 * block], gu_hbm.at[2 * block], gd_hbm.at[2 * block])
        targets = (gg_hbm.at[2 * block + 1], gu_hbm.at[2 * block + 1], gd_hbm.at[2 * block + 1])
        return [pltpu.make_async_remote_copy(
            src_ref=sources[k], dst_ref=targets[k], send_sem=d2d_send.at[block, k], recv_sem=d2d_recv.at[block, k],
            device_id=device(0, 0, 1), device_id_type=pl.DeviceIdType.MESH) for k in range(3)]

    plan = send_plan()
    waits, done = wait_plan()
    arrival = {(target, piece): (link, place, piece, source, target) for stage in plan for link, place, piece, source, target in stage}

    def service(point):
        for (dx, dy), pieces in waits[point]:
            for piece in pieces:
                ici_copy(*arrival[(block_of(dx, dy), piece)]).wait_recv()
        if point < len(plan):
            for entry in plan[point]:
                ici_copy(*entry).start()
        for dx, dy in done[point]:
            for copy in d2d_copies(block_of(dx, dy), (dx, dy) == (0, 0)):
                copy.start()

    loads = [
        (x_hbm, xs.at[1]), (norms_hbm, norms), (router_hbm, router), (ids_hbm, ids), (rope_hbm, rope),
        (wq_hbm.at[pl.ds(0, 512)], wqkv.at[0]), (wq_hbm.at[pl.ds(512, 512)], wqkv.at[1]), (wk_hbm, wqkv.at[2]), (wv_hbm, wqkv.at[3]),
        (wo_hbm.at[pl.ds(0, 512)], wo.at[0]), (wo_hbm.at[pl.ds(512, 512)], wo.at[1]),
    ]
    loads = [pltpu.make_async_copy(source, target, load_sem.at[k]) for k, (source, target) in enumerate(loads)]
    for copy in loads:
        copy.start()

    barrier = pltpu.get_barrier_semaphore()
    for peer in [device(*step, 0) for step in STEPS] + [device(0, 0, 1)]:
        pl.semaphore_signal(barrier, inc=1, device_id=peer, device_id_type=pl.DeviceIdType.MESH)
    pl.semaphore_wait(barrier, len(STEPS) + 1)
    service(0)

    def expert_copies(slot, sources):
        return [pltpu.make_async_copy(source, buffer.at[slot], w_sem.at[slot, k]) for k, (source, buffer) in enumerate(zip(sources, (wg, wu, wd)))]

    def prefetch(step, slot):
        @pl.when(step < ffn_steps)
        def _():
            cut = pl.ds(pl.multiple_of(step * hidden, hidden), hidden)
            for copy in expert_copies(slot, (fg_hbm.at[:, cut], fu_hbm.at[:, cut], fd_hbm.at[cut])):
                copy.start()

        @pl.when(step == ffn_steps)
        def _():
            for copy in expert_copies(slot, (eg_hbm.at[0], eu_hbm.at[0], ed_hbm.at[0])):
                copy.start()

        @pl.when((step > ffn_steps) & (step < steps))
        def _():
            rank = step - ffn_steps

            @pl.when(lax.rem(rank, 2) == 1)
            def _():
                for copy in d2d_copies(rank // 2, False):
                    copy.wait_recv()

            for copy in expert_copies(slot, (gg_hbm.at[rank], gu_hbm.at[rank], gd_hbm.at[rank])):
                copy.start()

    prefetch(0, 0)

    for copy in loads[:4]:
        copy.wait()
    ranks = lax.broadcasted_iota(jnp.int32, (experts, 1), 0)
    owner = jnp.zeros((experts, 1), jnp.int32)
    for block, (dx, dy) in enumerate(BLOCKS):
        chip = lax.rem(row - dy + SIDE, SIDE) * SIDE + lax.rem(col - dx + SIDE, SIDE)
        owner = jnp.where(ranks // 2 == block, chip, owner)
    owner = owner * 2 + lax.rem(core + lax.rem(ranks, 2), 2)
    ordered = (lax.broadcasted_iota(jnp.int32, (experts, experts), 1) == owner).astype(F32).astype(BF16)
    ordered = matmul(ordered, router[...]).astype(BF16)
    tile = 512

    def prologue(index, carry):
        part = pl.ds(pl.multiple_of(index * tile, tile), tile)
        values = xs[1, part, :].astype(F32)
        unit = values * norm_scale_of(values)
        tokens = (unit * norms[2:3, :]).astype(BF16)
        xs[0, part, :] = (unit * norms[0:1, :]).astype(BF16)
        xs[1, part, :] = tokens
        acc[part, :] = values
        logits = matmul_t(ordered, tokens)
        per_seq = seq // tile
        picks = ids[index // per_seq, :, pl.ds(pl.multiple_of(lax.rem(index, per_seq) * tile, tile), tile)]
        picked = picks[0:1, :] == owner
        for choice in range(1, picks.shape[0]):
            picked = picked | (picks[choice:choice + 1, :] == owner)
        top = jnp.max(jnp.where(picked, logits, -jnp.inf), axis=0, keepdims=True)
        powers = jnp.where(picked, jnp.exp(jnp.where(picked, logits, top) - top), 0.0)
        share = powers / jnp.sum(powers, axis=0, keepdims=True)
        share = jnp.concatenate([share, jnp.zeros((LANES - experts, tile), F32)], axis=0)
        gates[part, :] = share.T
        return carry

    lax.fori_loop(0, rows // tile, prologue, 0)
    for copy in loads[4:]:
        copy.wait()

    def sequence(micro_index, carry):
        base = pl.multiple_of(micro_index * seq, seq)

        @pl.when(micro_index == 1)
        def _():
            service(1)

        lane = lax.broadcasted_iota(jnp.int32, (seq, LANES), 1)
        first = lax.rem(lane, head) < head // 2
        low = lane < head
        cosine, sine = rope[0], rope[1]
        tokens = xs[0, pl.ds(base, seq), :]

        def rotated(values):
            swapped = jnp.where(first, pltpu.roll(values, LANES - head // 2, 1), pltpu.roll(values, head // 2, 1))
            return values * cosine + swapped * sine

        def doubled(values, target, pair):
            turned = pltpu.roll(values, head, 1)
            place = 2 * pair * LANES
            target[:, place:place + LANES] = jnp.where(low, values, turned).astype(BF16)
            target[:, place + LANES:place + 2 * LANES] = jnp.where(low, turned, values).astype(BF16)

        for block in range(4):
            flat = matmul_t(tokens, wqkv[block])
            for piece in range(512 // LANES):
                values = flat[:, piece * LANES:(piece + 1) * LANES]
                if block < 2:
                    place = block * 512 + piece * LANES
                    qs[:, place:place + LANES] = (rotated(values) * head ** -0.5).astype(BF16)
                elif block == 2:
                    doubled(rotated(values), ks, piece)
                else:
                    doubled(values, vs, piece)

        chunk = 256
        chunk_low = lax.broadcasted_iota(jnp.int32, (chunk, LANES), 1) < head
        inside = lax.rem(lax.broadcasted_iota(jnp.int32, (2 * chunk, chunk), 0), chunk) >= lax.broadcasted_iota(jnp.int32, (2 * chunk, chunk), 1)

        def columns(index):
            return pl.ds(pl.multiple_of(index * LANES, LANES), LANES)

        def score(index, parts, target):
            cols, place = columns(index), 0
            for part in parts:
                span = (part + 1) * chunk
                q_part = qs[part * chunk:span, cols]
                none = jnp.zeros_like(q_part)
                pair = jnp.concatenate([jnp.where(chunk_low, q_part, none), jnp.where(chunk_low, none, q_part)], axis=0)
                scores = matmul_t(pair, ks[:span, cols])
                edge = jnp.where(inside, scores[:, part * chunk:], -1e30)
                scores = edge if part == 0 else jnp.concatenate([scores[:, :part * chunk], edge], axis=1)
                target[:, place:place + span] = scores
                tops[part] = jnp.broadcast_to(jnp.max(scores, axis=1, keepdims=True), tops.shape[1:])
                place += span

        def soften(parts, origin, target):
            place = 0
            for part in parts:
                top = tops[part]
                total = jnp.zeros_like(top)
                for _ in range((part + 1) * chunk // LANES):
                    powers = jnp.exp(origin[:, place:place + LANES] - top)
                    total = total + powers
                    target[:, place:place + LANES] = powers.astype(BF16)
                    place += LANES
                sums[part] = jnp.broadcast_to(jnp.sum(total, axis=1, keepdims=True), sums.shape[1:])

        def mix(index, parts, origin):
            cols, place = columns(index), 0
            for part in parts:
                span = (part + 1) * chunk
                mixed = matmul(origin[:, place:place + span], vs[:span, cols]) / sums[part]
                os[part * chunk:span, cols] = jnp.where(chunk_low, mixed[:chunk], mixed[chunk:]).astype(BF16)
                place += span

        outer_parts, inner_parts = (0, 3), (1, 2)
        score(0, outer_parts, s_outer)

        def group(index, inner):
            score(index, inner_parts, s_inner)
            soften(outer_parts, s_outer, p_outer)
            mix(lax.rem(index + kv_heads - 1, kv_heads), inner_parts, p_inner)
            score(lax.rem(index + 1, kv_heads), outer_parts, s_outer)
            soften(inner_parts, s_inner, p_inner)
            mix(index, outer_parts, p_outer)
            return inner

        lax.fori_loop(0, kv_heads, group, 0)
        mix(kv_heads - 1, inner_parts, p_inner)

        def project(index, inner):
            local = pl.ds(pl.multiple_of(index * tile, tile), tile)
            part = pl.ds(pl.multiple_of(base + index * tile, tile), tile)
            added = matmul(os[local, :tile], wo[0]) + matmul(os[local, tile:], wo[1])
            after = (acc[part, :] + added).astype(BF16).astype(F32)
            acc[part, :] = after
            xs[0, part, :] = (after * norm_scale_of(after) * norms[1:2, :]).astype(BF16)
            return inner

        lax.fori_loop(0, seq // tile, project, 0)
        return carry

    lax.fori_loop(0, micro, sequence, 0)

    big = 1024
    lanes = lax.broadcasted_iota(jnp.int32, (big, LANES), 1)
    moments = {ffn_steps // 2: 2, ffn_steps + 4: 3, ffn_steps + 11: 4, ffn_steps + 18: 5}

    def ffn_step(step, carry):
        slot = lax.rem(step, 2)
        for copy in expert_copies(slot, (gg_hbm.at[0], gu_hbm.at[0], gd_hbm.at[0])):
            copy.wait()
        for moment, point in moments.items():
            @pl.when(step == moment)
            def _():
                service(point)

        prefetch(step + 1, 1 - slot)
        dense = step < ffn_steps
        source = (step + steps - ffn_steps) // steps
        gate_w, up_w, down_w = wg.at[slot], wu.at[slot], wd.at[slot]

        def rows_step(index, inner):
            part = pl.ds(pl.multiple_of(index * big, big), big)
            tokens = xs[source, part, :]
            weight = jnp.sum(jnp.where(lanes == step - ffn_steps, gates[part, :], 0.0), axis=1, keepdims=True)
            weight = jnp.where(dense, 1.0, weight)
            gate_act = matmul(tokens, gate_w[...])
            up_act = matmul(tokens, up_w[...])
            mixed = (jax.nn.silu(gate_act) * up_act).astype(BF16)
            down = matmul(mixed, down_w[...])
            down = jnp.where(dense, down, down.astype(BF16).astype(F32))
            acc[part, :] += jnp.where(weight > 0.0, weight * down, 0.0)
            return inner

        lax.fori_loop(0, rows // big, rows_step, 0)
        return carry

    lax.fori_loop(0, steps, ffn_step, 0)

    def store(index):
        part = pl.ds(index * tile, tile)
        return pltpu.make_async_copy(xs.at[0, part], out_hbm.at[part], out_sem.at[index])

    for index in range(rows // tile):
        xs[0, index * tile:(index + 1) * tile, :] = acc[index * tile:(index + 1) * tile, :].astype(BF16)
        store(index).start()
    for stage in plan:
        for entry in stage:
            ici_copy(*entry).wait_send()
    for block in range(len(BLOCKS)):
        for copy in d2d_copies(block, block == 0):
            copy.wait_send()
    for index in range(rows // tile):
        store(index).wait()


def rope_tables(seq, head):
    half = head // 2
    freqs = np.float32(ROPE_BASE) ** (-np.arange(half, dtype=np.float32) * np.float32(2.0) / np.float32(head))
    angles = np.arange(seq, dtype=np.float32)[:, None] * freqs.astype(np.float32)[None, :]
    cosine = np.cos(angles.astype(np.float64)).astype(np.float32)
    sine = np.sin(angles.astype(np.float64)).astype(np.float32)
    times = LANES // head
    return np.stack([np.tile(np.concatenate([cosine, cosine], 1), (1, times)), np.tile(np.concatenate([-sine, sine], 1), (1, times))])


def solution(mesh):
    tok_spec = P(None, ('dp', 'ep'), None, None)
    rep_one = P(None)
    rep_two = P(None, None)
    rep_three = P(None, None, None)
    expert_spec = P('ep', None, None)
    assert mesh.shape['ep'] == 2 * SIDE * SIDE

    def local_program(resid_in, expert_idx, expert_slot, w_query, w_key, w_value, w_out, w_gate, w_up, w_down, w_router, norm_attn, norm_ffn, norm_moe, expert_gate, expert_up, expert_down):
        micro, seqs, seq, width = resid_in.shape
        choices = expert_idx.shape[-1]
        heads, head = w_query.shape[1:]
        kv_heads = w_key.shape[1]
        hidden = expert_gate.shape[2]
        experts = 2 * len(BLOCKS)
        rows = micro * seqs * seq
        ids = expert_idx.transpose(0, 1, 3, 2).reshape(micro * seqs, choices, seq)
        norms = jnp.stack([norm_attn, norm_ffn, norm_moe]).astype(F32)
        rope = jnp.asarray(rope_tables(seq, head))
        anywhere = pl.BlockSpec(memory_space=pl.ANY)
        operands = (
            resid_in.reshape(rows, width), ids, w_router.T, norms, rope,
            w_query.transpose(1, 2, 0).reshape(heads * head, width), w_key.transpose(1, 2, 0).reshape(kv_heads * head, width),
            w_value.transpose(1, 2, 0).reshape(kv_heads * head, width), w_out.reshape(heads * head, width),
            w_gate, w_up, w_down, expert_gate, expert_up, expert_down)
        flops = rows * width * 2 * (3 * hidden * experts + 3 * w_gate.shape[1] + 3 * heads * head)
        out = pl.pallas_call(
            functools.partial(fused_kernel, (rows, width, seq, hidden, heads, kv_heads, head)),
            out_shape=(
                jax.ShapeDtypeStruct((rows, width), BF16),
                jax.ShapeDtypeStruct((experts, width, hidden), BF16),
                jax.ShapeDtypeStruct((experts, width, hidden), BF16),
                jax.ShapeDtypeStruct((experts, hidden, width), BF16)),
            in_specs=[anywhere] * len(operands),
            out_specs=[anywhere] * 4,
            scratch_shapes=[
                pltpu.VMEM((2, rows, width), BF16),
                pltpu.VMEM((rows, width), F32),
                pltpu.VMEM((rows, LANES), F32),
                pltpu.VMEM((seq, heads * head), BF16),
                pltpu.VMEM((seq, kv_heads * LANES), BF16),
                pltpu.VMEM((seq, kv_heads * LANES), BF16),
                pltpu.VMEM((seq, heads * head), BF16),
                *[pltpu.VMEM((512, 1280), kind) for kind in (F32, F32, BF16, BF16)],
                *[pltpu.VMEM((4, 512, LANES), F32) for _ in range(2)],
                pltpu.VMEM((micro * seqs, choices, seq), jnp.int32),
                pltpu.VMEM((experts, width), BF16),
                pltpu.VMEM((3, width), F32),
                pltpu.VMEM((2, seq, LANES), F32),
                pltpu.VMEM((4, 512, width), BF16),
                pltpu.VMEM((2, 512, width), BF16),
                *[pltpu.VMEM((2,) + shape, BF16) for shape in ((width, hidden), (width, hidden), (hidden, width))],
                *[pltpu.SemaphoreType.DMA(shape) for shape in ((11,), (2, 3), (4,), (4, 15), (16, 4), (16, 3), (16, 3))],
            ],
            compiler_params=pltpu.CompilerParams(collective_id=0, has_side_effects=True, vmem_limit_bytes=62 * 1024 * 1024),
            cost_estimate=pl.CostEstimate(flops=flops, bytes_accessed=experts * 6 * width * hidden, transcendentals=0),
        )(*operands)[0]
        return out.reshape(resid_in.shape)

    return jax.shard_map(local_program, mesh=mesh, in_specs=(tok_spec, tok_spec, tok_spec, rep_three, rep_three, rep_three, rep_three, rep_two, rep_two, rep_two, rep_two, rep_one, rep_one, rep_one, expert_spec, expert_spec, expert_spec), out_specs=tok_spec, check_vma=False)
```

```python
import functools
import math

import jax
import jax.numpy as jnp
import numpy as np
from jax import lax
from jax.experimental import pallas as pl
from jax.experimental.pallas import tpu as pltpu
from jax.sharding import PartitionSpec as P

EPS = 1e-6
ROPE_BASE = 10000.0
LANES = 128
F32 = jnp.float32
BF16 = jnp.bfloat16

UNIT = 8
TILE = 256
STATIC = 16

SIDE = 4
NEAR = (1, 3)
BLOCKS = (
    (0, 0), *[(a, 0) for a in NEAR], *[(0, a) for a in NEAR], *[(a, b) for a in NEAR for b in NEAR],
    *[place for a in (0, *NEAR) for place in ((2, a), (a, 2))], (2, 2))
STEPS = ((1, 0), (-1, 0), (0, 1), (0, -1))
GATE, UP, LOW, HIGH, LOW_A, LOW_B, HIGH_A, HIGH_B = range(8)
X_FIRST, Y_FIRST = (GATE, LOW), (UP, HIGH)
ALL = (*X_FIRST, *Y_FIRST)
LAST = ((1, 2), (3, 2), (2, 1), (2, 3))


def block_of(dx, dy):
    return BLOCKS.index((dx % SIDE, dy % SIDE))


def send_plan():
    plan = [[] for _ in range(5)]
    used = [0] * len(STEPS)

    def send(service, link, pieces, dx, dy):
        sx, sy = STEPS[link]
        for piece in pieces:
            plan[service].append((link, used[link], piece, block_of(dx, dy), block_of(dx + sx, dy + sy)))
            used[link] += 1

    def spread(service, dx, dy):
        pieces, start = (X_FIRST, 2) if dy == 0 else (Y_FIRST, 0)
        send(service, start, pieces, dx, dy)
        send(service, start + 1, pieces[::-1], dx, dy)

    def relay(service, pieces, blocks):
        for link, (piece, block) in enumerate(zip(pieces, blocks)):
            send(service, link, (piece,), *block)

    for link, order in enumerate((X_FIRST, X_FIRST[::-1], Y_FIRST, Y_FIRST[::-1])):
        send(0, link, order, 0, 0)
    for link, order in enumerate((Y_FIRST, Y_FIRST[::-1], X_FIRST, X_FIRST[::-1])):
        send(0, link, order, 0, 0)

    relay(1, (GATE, LOW, UP, HIGH), BLOCKS[1:5])
    for a in NEAR:
        spread(1, 0, a)
        spread(1, a, 0)
    relay(2, (HIGH, UP, LOW, GATE), BLOCKS[1:5])
    spread(2, 0, 2)
    spread(2, 2, 0)
    for a in NEAR:
        relay(3, (UP, HIGH, GATE, LOW), ((1, a), (3, a), (a, 1), (a, 3)))
    relay(4, (HIGH_A, UP, LOW_A, GATE), LAST)
    for link, piece in ((1, HIGH_B), (3, LOW_B)):
        send(4, link, (piece,), *LAST[link])
    return plan


def wait_plan():
    rows, cols = [(a, 0) for a in NEAR], [(0, a) for a in NEAR]
    far_rows, far_cols = [(2, a) for a in NEAR], [(a, 2) for a in NEAR]

    def need(first, second):
        return [(block, X_FIRST) for block in first] + [(block, Y_FIRST) for block in second]

    return [
        [],
        need(rows, cols),
        need(cols + [(2, 0)], rows + [(0, 2)]),
        [((a, b), ALL) for a in NEAR for b in NEAR],
        need([(0, 2)] + far_rows, [(2, 0)] + far_cols),
        need(far_cols, far_rows),
        [((2, 2), (UP, GATE, HIGH_A, LOW_A, HIGH_B, LOW_B))],
    ]


def matmul(left, right):
    return jnp.dot(left, right, preferred_element_type=F32)


def matmul_t(left, right):
    return lax.dot_general(left, right, (((1,), (1,)), ((), ())), preferred_element_type=F32)


def norm_scale_of(values):
    return lax.rsqrt(jnp.mean(values * values, axis=-1, keepdims=True) + EPS)


def fused_kernel(
    dims,
    x_hbm, ids_hbm, router_hbm, norms_hbm, rope_hbm, wq_hbm, wk_hbm, wv_hbm, wo_hbm, fg_hbm, fu_hbm, fd_hbm, eg_hbm, eu_hbm, ed_hbm,
    base_hbm, tokens_hbm, picks_hbm, shares_hbm, counts_hbm, gg_hbm, gu_hbm, gd_hbm,
    picks, shares, counts, xs, acc, gates, qs, ks, vs, os, s_outer, s_inner, p_outer, p_inner, tops, sums, ids, router, norms, rope, wqkv, wo, wg, wu, wd,
    load_sem, w_sem, out_sem, ici_send, ici_recv, d2d_send, d2d_recv,
):
    rows, width, seq, hidden, heads, kv_heads, head = dims
    micro = rows // seq
    half = hidden // 2
    experts = 2 * len(BLOCKS)
    ffn_steps = fg_hbm.shape[1] // hidden
    steps = ffn_steps + STATIC
    late = experts - STATIC
    me = lax.axis_index('ep')
    core = lax.rem(me, 2)
    col = lax.rem(me // 2, SIDE)
    row = me // (2 * SIDE)

    def device(dx, dy, flip):
        cx = lax.rem(col + dx + SIDE, SIDE)
        cy = lax.rem(row + dy + SIDE, SIDE)
        return {'ep': (cy * SIDE + cx) * 2 + lax.rem(core + flip, 2)}

    def cut(piece, gate, up, down):
        if piece < LOW:
            return (gate, up)[piece]
        start, size = {LOW: (0, 2), HIGH: (2, 2), LOW_A: (0, 1), LOW_B: (1, 1), HIGH_A: (2, 1), HIGH_B: (3, 1)}[piece]
        return down.at[pl.ds(start * hidden // 4, size * hidden // 4)]

    def piece_ref(block, piece):
        if block == 0:
            return cut(piece, eg_hbm.at[0], eu_hbm.at[0], ed_hbm.at[0])
        return slot_ref(2 * block, piece)

    def slot_ref(slot, piece):
        return cut(piece, gg_hbm.at[slot], gu_hbm.at[slot], gd_hbm.at[slot])

    def ici_copy(link, place, piece, source, target):
        return pltpu.make_async_remote_copy(
            src_ref=piece_ref(source, piece), dst_ref=slot_ref(2 * target, piece),
            send_sem=ici_send.at[link, place], recv_sem=ici_recv.at[target, piece],
            device_id=device(*STEPS[link], 0), device_id_type=pl.DeviceIdType.MESH)

    def d2d_copy(block, piece, source):
        return pltpu.make_async_remote_copy(
            src_ref=source, dst_ref=slot_ref(2 * block + 1, piece), send_sem=d2d_send.at[block, piece], recv_sem=d2d_recv.at[block, piece],
            device_id=device(0, 0, 1), device_id_type=pl.DeviceIdType.MESH)

    def pieces_of(block):
        return waits[-1][0][1] if block == len(BLOCKS) - 1 else ALL

    def d2d_wait(block, pieces=ALL):
        for piece in pieces:
            d2d_copy(block, piece, slot_ref(2 * block + 1, piece)).wait_recv()

    plan = send_plan()
    waits = wait_plan()
    arrival = {(target, piece): (link, place, piece, source, target) for stage in plan for link, place, piece, source, target in stage}

    def service(point):
        landed = [(block_of(*block), piece) for block, pieces in waits[point] for piece in pieces]
        for block, piece in landed:
            ici_copy(*arrival[block, piece]).wait_recv()
            if point >= len(plan):
                d2d_copy(block, piece, piece_ref(block, piece)).start()
        if point < len(plan):
            for entry in plan[point]:
                ici_copy(*entry).start()
            for block, piece in landed if point else [(0, piece) for piece in ALL]:
                d2d_copy(block, piece, piece_ref(block, piece)).start()

    loads = [
        (x_hbm, xs.at[1]), (norms_hbm, norms), (router_hbm, router), (ids_hbm, ids), (rope_hbm, rope),
        (wq_hbm.at[pl.ds(0, 512)], wqkv.at[0]), (wq_hbm.at[pl.ds(512, 512)], wqkv.at[1]), (wk_hbm, wqkv.at[2]), (wv_hbm, wqkv.at[3]),
        (wo_hbm.at[pl.ds(0, 512)], wo.at[0]), (wo_hbm.at[pl.ds(512, 512)], wo.at[1]),
    ]
    loads = [pltpu.make_async_copy(source, target, load_sem.at[k]) for k, (source, target) in enumerate(loads)]
    for copy in loads:
        copy.start()

    barrier = pltpu.get_barrier_semaphore()
    for peer in [device(*step, 0) for step in STEPS] + [device(0, 0, 1)]:
        pl.semaphore_signal(barrier, inc=1, device_id=peer, device_id_type=pl.DeviceIdType.MESH)
    pl.semaphore_wait(barrier, len(STEPS) + 1)
    service(0)

    def expert_copies(slot, sources):
        return [pltpu.make_async_copy(source, buffer.at[slot], w_sem.at[slot, k]) for k, (source, buffer) in enumerate(zip(sources, (wg, wu, wd)))]

    def prefetch(step, slot):
        @pl.when(step < ffn_steps)
        def _():
            cut = pl.ds(pl.multiple_of(step * hidden, hidden), hidden)
            for copy in expert_copies(slot, (fg_hbm.at[:, cut], fu_hbm.at[:, cut], fd_hbm.at[cut])):
                copy.start()

        @pl.when(step == ffn_steps)
        def _():
            for copy in expert_copies(slot, (eg_hbm.at[0], eu_hbm.at[0], ed_hbm.at[0])):
                copy.start()

        @pl.when((step > ffn_steps) & (step < steps))
        def _():
            rank = step - ffn_steps

            @pl.when(lax.rem(rank, 2) == 1)
            def _():
                d2d_wait(rank // 2)

            for copy in expert_copies(slot, (gg_hbm.at[rank], gu_hbm.at[rank], gd_hbm.at[rank])):
                copy.start()

    prefetch(0, 0)

    for copy in loads[:4]:
        copy.wait()
    ranks = lax.broadcasted_iota(jnp.int32, (experts, 1), 0)
    owner = jnp.zeros((experts, 1), jnp.int32)
    for block, (dx, dy) in enumerate(BLOCKS):
        chip = lax.rem(row - dy + SIDE, SIDE) * SIDE + lax.rem(col - dx + SIDE, SIDE)
        owner = jnp.where(ranks // 2 == block, chip, owner)
    owner = owner * 2 + lax.rem(core + lax.rem(ranks, 2), 2)
    ordered = (lax.broadcasted_iota(jnp.int32, (experts, experts), 1) == owner).astype(F32).astype(BF16)
    ordered = matmul(ordered, router[...]).astype(BF16)
    tile = 512
    tile_lanes = lax.broadcasted_iota(jnp.int32, (tile, LANES), 1)
    spots = lax.broadcasted_iota(jnp.int32, (tile, tile), 1)
    earlier = (lax.broadcasted_iota(jnp.int32, (tile, tile), 0) > spots).astype(F32).astype(BF16)
    spots = spots.astype(F32)
    quarters = tile // LANES
    pitch = rows // LANES + 1
    list_lines = (2 * tile + TILE) // LANES
    picks[...] = jnp.zeros_like(picks)
    shares[pl.ds(0, experts, stride=pitch), :] = jnp.zeros((experts, LANES), F32)

    def prologue(index, so_far):
        part = pl.ds(pl.multiple_of(index * tile, tile), tile)
        values = xs[1, part, :].astype(F32)
        unit = values * norm_scale_of(values)
        tokens = (unit * norms[2:3, :]).astype(BF16)
        xs[0, part, :] = (unit * norms[0:1, :]).astype(BF16)
        xs[1, part, :] = tokens
        acc[part, :] = values
        logits = matmul_t(ordered, tokens)
        per_seq = seq // tile
        wanted = ids[index // per_seq, :, pl.ds(pl.multiple_of(lax.rem(index, per_seq) * tile, tile), tile)]
        picked = wanted[0:1, :] == owner
        for choice in range(1, wanted.shape[0]):
            picked = picked | (wanted[choice:choice + 1, :] == owner)
        top = jnp.max(jnp.where(picked, logits, -jnp.inf), axis=0, keepdims=True)
        powers = jnp.where(picked, jnp.exp(jnp.where(picked, logits, top) - top), 0.0)
        share = powers / jnp.sum(powers, axis=0, keepdims=True)
        for lane_cut in range(quarters):
            shares[pl.ds(1 + index * quarters + lane_cut, experts, stride=pitch), :] = share[:, lane_cut * LANES:(lane_cut + 1) * LANES]
        share = jnp.concatenate([share, jnp.zeros((LANES - experts, tile), F32)], axis=0)
        share = share.T
        gates[part, :] = share

        chosen = share > 0.0
        ones = chosen.astype(F32)
        place = jnp.where(chosen, matmul(earlier, ones.astype(BF16)) + so_far, -1.0)
        so_far = so_far + jnp.sum(ones, axis=0, keepdims=True)
        token = lax.broadcasted_iota(jnp.int32, (tile, tile), 0) + (index * tile + 1)
        token = token.astype(F32)

        def listed(rank, inner):
            mine = tile_lanes == rank + STATIC
            spot = jnp.sum(jnp.where(mine, place, 0.0), axis=1, keepdims=True)
            for half in range(2):
                found = jnp.sum(jnp.where(spot - half * tile == spots, token, 0.0), axis=0, keepdims=True).astype(jnp.int32)
                for lane_cut in range(quarters):
                    line = pl.ds(rank * list_lines + half * quarters + lane_cut, 1)
                    picks[line, :] += found[:, lane_cut * LANES:(lane_cut + 1) * LANES]
            return inner

        lax.fori_loop(0, late, listed, 0)
        return so_far

    counts[...] = jnp.broadcast_to(lax.fori_loop(0, rows // tile, prologue, jnp.zeros((1, LANES), F32)), counts.shape).astype(jnp.int32)
    results = [(xs.at[1], tokens_hbm), (picks, picks_hbm), (shares, shares_hbm), (counts, counts_hbm), (acc, base_hbm)]
    results = [pltpu.make_async_copy(source, target, out_sem.at[k]) for k, (source, target) in enumerate(results)]
    for copy in results[:-1]:
        copy.start()
    for copy in loads[4:]:
        copy.wait()

    def sequence(micro_index, carry):
        base = pl.multiple_of(micro_index * seq, seq)

        @pl.when(micro_index == 1)
        def _():
            service(1)

        lane = lax.broadcasted_iota(jnp.int32, (seq, LANES), 1)
        first = lax.rem(lane, head) < head // 2
        low = lane < head
        cosine, sine = rope[0], rope[1]
        tokens = xs[0, pl.ds(base, seq), :]

        def rotated(values):
            swapped = jnp.where(first, pltpu.roll(values, LANES - head // 2, 1), pltpu.roll(values, head // 2, 1))
            return values * cosine + swapped * sine

        def doubled(values, target, pair):
            turned = pltpu.roll(values, head, 1)
            place = 2 * pair * LANES
            target[:, place:place + LANES] = jnp.where(low, values, turned).astype(BF16)
            target[:, place + LANES:place + 2 * LANES] = jnp.where(low, turned, values).astype(BF16)

        for block in range(4):
            flat = matmul_t(tokens, wqkv[block])
            for piece in range(512 // LANES):
                values = flat[:, piece * LANES:(piece + 1) * LANES]
                if block < 2:
                    place = block * 512 + piece * LANES
                    qs[:, place:place + LANES] = (rotated(values) * head ** -0.5).astype(BF16)
                elif block == 2:
                    doubled(rotated(values), ks, piece)
                else:
                    doubled(values, vs, piece)

        chunk = 256
        chunk_low = lax.broadcasted_iota(jnp.int32, (chunk, LANES), 1) < head
        inside = lax.rem(lax.broadcasted_iota(jnp.int32, (2 * chunk, chunk), 0), chunk) >= lax.broadcasted_iota(jnp.int32, (2 * chunk, chunk), 1)

        def columns(index):
            return pl.ds(pl.multiple_of(index * LANES, LANES), LANES)

        def score(index, parts, target):
            cols, place = columns(index), 0
            for part in parts:
                span = (part + 1) * chunk
                q_part = qs[part * chunk:span, cols]
                none = jnp.zeros_like(q_part)
                pair = jnp.concatenate([jnp.where(chunk_low, q_part, none), jnp.where(chunk_low, none, q_part)], axis=0)
                scores = matmul_t(pair, ks[:span, cols])
                edge = jnp.where(inside, scores[:, part * chunk:], -1e30)
                scores = edge if part == 0 else jnp.concatenate([scores[:, :part * chunk], edge], axis=1)
                target[:, place:place + span] = scores
                tops[part] = jnp.broadcast_to(jnp.max(scores, axis=1, keepdims=True), tops.shape[1:])
                place += span

        def soften(parts, origin, target):
            place = 0
            for part in parts:
                top = tops[part]
                total = jnp.zeros_like(top)
                for _ in range((part + 1) * chunk // LANES):
                    powers = jnp.exp(origin[:, place:place + LANES] - top)
                    total = total + powers
                    target[:, place:place + LANES] = powers.astype(BF16)
                    place += LANES
                sums[part] = jnp.broadcast_to(jnp.sum(total, axis=1, keepdims=True), sums.shape[1:])

        def mix(index, parts, origin):
            cols, place = columns(index), 0
            for part in parts:
                span = (part + 1) * chunk
                mixed = matmul(origin[:, place:place + span], vs[:span, cols]) / sums[part]
                os[part * chunk:span, cols] = jnp.where(chunk_low, mixed[:chunk], mixed[chunk:]).astype(BF16)
                place += span

        outer_parts, inner_parts = (0, 3), (1, 2)
        score(0, outer_parts, s_outer)

        def group(index, inner):
            score(index, inner_parts, s_inner)
            soften(outer_parts, s_outer, p_outer)
            mix(lax.rem(index + kv_heads - 1, kv_heads), inner_parts, p_inner)
            score(lax.rem(index + 1, kv_heads), outer_parts, s_outer)
            soften(inner_parts, s_inner, p_inner)
            mix(index, outer_parts, p_outer)
            return inner

        lax.fori_loop(0, kv_heads, group, 0)
        mix(kv_heads - 1, inner_parts, p_inner)

        def project(index, inner):
            local = pl.ds(pl.multiple_of(index * tile, tile), tile)
            part = pl.ds(pl.multiple_of(base + index * tile, tile), tile)
            added = matmul(os[local, :tile], wo[0]) + matmul(os[local, tile:], wo[1])
            after = (acc[part, :] + added).astype(BF16).astype(F32)
            acc[part, :] = after
            xs[0, part, :] = (after * norm_scale_of(after) * norms[1:2, :]).astype(BF16)
            return inner

        lax.fori_loop(0, seq // tile, project, 0)
        return carry

    lax.fori_loop(0, micro, sequence, 0)

    big = 1024
    lanes = lax.broadcasted_iota(jnp.int32, (big, LANES), 1)
    moments = {4: 2, 13: 3, 20: 4, 23: 5}

    def ffn_step(step, carry):
        slot = lax.rem(step, 2)
        for copy in expert_copies(slot, (gg_hbm.at[0], gu_hbm.at[0], gd_hbm.at[0])):
            copy.wait()
        for moment, point in moments.items():
            @pl.when(step == moment)
            def _():
                service(point)

        prefetch(step + 1, 1 - slot)
        dense = step < ffn_steps
        source = (step + steps - ffn_steps) // steps
        gate_w, up_w, down_w = wg.at[slot], wu.at[slot], wd.at[slot]

        def rows_step(index, inner):
            part = pl.ds(pl.multiple_of(index * big, big), big)
            tokens = xs[source, part, :]
            weight = jnp.sum(jnp.where(lanes == step - ffn_steps, gates[part, :], 0.0), axis=1, keepdims=True)
            weight = jnp.where(dense, 1.0, weight)
            gate_act = matmul(tokens, gate_w[...])
            up_act = matmul(tokens, up_w[...])
            mixed = (jax.nn.silu(gate_act) * up_act).astype(BF16)
            down = matmul(mixed, down_w[...])
            down = jnp.where(dense, down, down.astype(BF16).astype(F32))
            acc[part, :] += jnp.where(weight > 0.0, weight * down, 0.0)
            return inner

        lax.fori_loop(0, rows // big, rows_step, 0)
        return carry

    lax.fori_loop(0, steps, ffn_step, 0)

    results[-1].start()
    service(len(waits) - 1)
    for block in range(STATIC // 2, len(BLOCKS)):
        d2d_wait(block, pieces_of(block))
    for stage in plan:
        for entry in stage:
            ici_copy(*entry).wait_send()
    for block in range(len(BLOCKS)):
        for piece in pieces_of(block):
            d2d_copy(block, piece, piece_ref(block, piece)).wait_send()
    for copy in results:
        copy.wait()


def compact_kernel(
    dims,
    picks_hbm, shares_hbm, counts_hbm, tokens_hbm, base_hbm, gg_hbm, gu_hbm, gd_hbm,
    out_hbm,
    picks, shares, counts, tokens, base, table, total, packed, lhs, result, wg, wu, wd,
    load_sem, w_sem, out_sem,
):
    rows, width, first, ranks = dims
    list_size = 1024 + TILE
    parts = width // LANES
    experts = first + ranks
    loads = [pltpu.make_async_copy(source, target, load_sem.at[k]) for k, (source, target) in enumerate((
        (tokens_hbm, tokens), (picks_hbm, picks), (shares_hbm, shares), (counts_hbm, counts), (base_hbm, base)))]
    for copy in loads:
        copy.start()

    def weights(rank, slot):
        return [pltpu.make_async_copy(source.at[first + rank], buffer.at[slot], w_sem.at[slot, k])
                for k, (source, buffer) in enumerate(((gg_hbm, wg), (gu_hbm, wu), (gd_hbm, wd)))]

    for copy in weights(0, 0):
        copy.start()

    loads[0].wait()
    table[0] = jnp.zeros((parts, LANES), F32)
    total[0] = jnp.zeros((parts, LANES), F32)
    flat = table.reshape((rows + 1) * parts, LANES)
    step_rows = 512

    def spread(index, carry):
        start = pl.multiple_of(index * step_rows, step_rows)
        values = tokens[pl.ds(start, step_rows), :].astype(F32)
        for part in range(parts):
            flat[pl.ds(parts + start * parts + part, step_rows, stride=parts), :] = values[:, part * LANES:(part + 1) * LANES]
        total[pl.ds(1 + start, step_rows)] = jnp.zeros((step_rows, parts, LANES), F32)
        return carry

    lax.fori_loop(0, rows // step_rows, spread, 0)
    for copy in loads[1:4]:
        copy.wait()

    def tiles_of(rank):
        return jnp.maximum((counts[0, first + rank] + TILE - 1) // TILE, 1)

    lot = rows + LANES

    def gather(rank, tile):
        start = rank * list_size + tile * TILE
        for place in range(TILE):
            spots = pl.ds(place // UNIT * UNIT * parts + place % UNIT, parts, stride=UNIT)
            packed.reshape(TILE * parts, LANES)[spots, :] = table[picks[start + place]]

    def scatter(rank, tile):
        start = rank * list_size + tile * TILE
        lead = (first + rank) * lot + LANES - 1
        for group in range(0, TILE, UNIT):
            rows_of = [picks[start + group + place] for place in range(UNIT)]
            sums = [total[row] + shares[lead + row] * result[group + place] for place, row in enumerate(rows_of)]
            for row, value in zip(rows_of, sums):
                total[row] = value

    count = lax.fori_loop(0, ranks, lambda rank, so_far: so_far + tiles_of(rank), 0)
    gather(0, 0)

    def tile_step(index, carry):
        rank, tile, last_rank, last_tile = carry
        slot = lax.rem(rank, 2)

        @pl.when(tile == 0)
        def _():
            for copy in weights(rank, slot):
                copy.wait()

            @pl.when(rank + 1 < ranks)
            def _():
                for copy in weights(rank + 1, 1 - slot):
                    copy.start()

        more = tile + 1 < tiles_of(rank)
        next_rank = jnp.where(more, rank, rank + 1)
        next_tile = jnp.where(more, tile + 1, 0)
        for part in range(parts):
            lhs[:, part * LANES:(part + 1) * LANES] = packed[:, part].reshape(TILE, LANES).astype(BF16)
        scatter(last_rank, last_tile)
        gather(next_rank, next_tile)
        gate_act = matmul(lhs[...], wg[slot])
        up_act = matmul(lhs[...], wu[slot])
        mixed = (jax.nn.silu(gate_act) * up_act).astype(BF16)
        down = matmul(mixed, wd[slot]).astype(BF16).astype(F32)
        for part in range(parts):
            result.reshape(TILE * parts, LANES)[pl.ds(part, TILE, stride=parts), :] = down[:, part * LANES:(part + 1) * LANES]
        return next_rank, next_tile, rank, tile

    _, _, last_rank, last_tile = lax.fori_loop(0, count, tile_step, (jnp.int32(0), jnp.int32(0), jnp.int32(ranks), jnp.int32(0)))
    scatter(last_rank, last_tile)
    loads[4].wait()
    sums_of = total.reshape((rows + 1) * parts, LANES)

    def store(index):
        part = pl.ds(index * step_rows, step_rows)
        return pltpu.make_async_copy(tokens.at[part], out_hbm.at[part], out_sem.at[index])

    for index in range(rows // step_rows):
        span = slice(index * step_rows, (index + 1) * step_rows)
        for part in range(parts):
            cols = slice(part * LANES, (part + 1) * LANES)
            moe = sums_of[pl.ds(parts + index * step_rows * parts + part, step_rows, stride=parts), :]
            tokens[span, cols] = (base[span, cols] + moe).astype(BF16)
        store(index).start()
    for index in range(rows // step_rows):
        store(index).wait()

def rope_tables(seq, head):
    half = head // 2
    freqs = np.float32(ROPE_BASE) ** (-np.arange(half, dtype=np.float32) * np.float32(2.0) / np.float32(head))
    angles = np.arange(seq, dtype=np.float32)[:, None] * freqs.astype(np.float32)[None, :]
    cosine = np.cos(angles.astype(np.float64)).astype(np.float32)
    sine = np.sin(angles.astype(np.float64)).astype(np.float32)
    times = LANES // head
    return np.stack([np.tile(np.concatenate([cosine, cosine], 1), (1, times)), np.tile(np.concatenate([-sine, sine], 1), (1, times))])


def solution(mesh):
    tok_spec = P(None, ('dp', 'ep'), None, None)
    rep_one = P(None)
    rep_two = P(None, None)
    rep_three = P(None, None, None)
    expert_spec = P('ep', None, None)
    assert mesh.shape['ep'] == 2 * SIDE * SIDE

    def local_program(resid_in, expert_idx, expert_slot, w_query, w_key, w_value, w_out, w_gate, w_up, w_down, w_router, norm_attn, norm_ffn, norm_moe, expert_gate, expert_up, expert_down):
        micro, seqs, seq, width = resid_in.shape
        choices = expert_idx.shape[-1]
        heads, head = w_query.shape[1:]
        kv_heads = w_key.shape[1]
        hidden = expert_gate.shape[2]
        experts = 2 * len(BLOCKS)
        rows = micro * seqs * seq
        ids = expert_idx.transpose(0, 1, 3, 2).reshape(micro * seqs, choices, seq)
        norms = jnp.stack([norm_attn, norm_ffn, norm_moe]).astype(F32)
        rope = jnp.asarray(rope_tables(seq, head))
        anywhere = pl.BlockSpec(memory_space=pl.ANY)
        operands = (
            resid_in.reshape(rows, width), ids, w_router.T, norms, rope,
            w_query.transpose(1, 2, 0).reshape(heads * head, width), w_key.transpose(1, 2, 0).reshape(kv_heads * head, width),
            w_value.transpose(1, 2, 0).reshape(kv_heads * head, width), w_out.reshape(heads * head, width),
            w_gate, w_up, w_down, expert_gate, expert_up, expert_down)
        flops = rows * width * 2 * (3 * hidden * experts + 3 * w_gate.shape[1] + 3 * heads * head)
        late = experts - STATIC
        lists = ((late + 1) * (1024 + TILE) // LANES, LANES)
        lots = (experts * (rows // LANES + 1), LANES)
        weight_shapes = ((width, hidden), (width, hidden), (hidden, width))
        double = [pltpu.VMEM((2,) + shape, BF16) for shape in weight_shapes]
        base, tokens, picks, shares, counts, gate_all, up_all, down_all = pl.pallas_call(
            functools.partial(fused_kernel, (rows, width, seq, hidden, heads, kv_heads, head)),
            out_shape=tuple(jax.ShapeDtypeStruct(shape, kind) for shape, kind in (
                ((rows, width), F32), ((rows, width), BF16), (lists, jnp.int32), (lots, F32), ((UNIT, LANES), jnp.int32),
                *[((experts,) + shape, BF16) for shape in weight_shapes])),
            in_specs=[anywhere] * len(operands),
            out_specs=[anywhere] * 8,
            scratch_shapes=[
                pltpu.VMEM(lists, jnp.int32),
                pltpu.VMEM(lots, F32),
                pltpu.VMEM((UNIT, LANES), jnp.int32),
                pltpu.VMEM((2, rows, width), BF16),
                pltpu.VMEM((rows, width), F32),
                pltpu.VMEM((rows, LANES), F32),
                *[pltpu.VMEM((seq, heads * head), BF16) for _ in range(4)],
                *[pltpu.VMEM((512, 1280), kind) for kind in (F32, F32, BF16, BF16)],
                *[pltpu.VMEM((4, 512, LANES), F32) for _ in range(2)],
                pltpu.VMEM((micro * seqs, choices, seq), jnp.int32),
                pltpu.VMEM((experts, width), BF16),
                pltpu.VMEM((3, width), F32),
                pltpu.VMEM((2, seq, LANES), F32),
                pltpu.VMEM((4, 512, width), BF16),
                pltpu.VMEM((2, 512, width), BF16),
                *double,
                *[pltpu.SemaphoreType.DMA(shape) for shape in ((11,), (2, 3), (5,), (4, 16), (16, 8), (16, 8), (16, 8))],
            ],
            compiler_params=pltpu.CompilerParams(collective_id=0, has_side_effects=True, vmem_limit_bytes=62 * 1024 * 1024),
            cost_estimate=pl.CostEstimate(flops=flops, bytes_accessed=experts * 6 * width * hidden, transcendentals=0),
        )(*operands)
        parts = width // LANES
        picks, shares = picks.reshape(-1), shares.reshape(-1)
        staged = pltpu.VMEM((TILE // UNIT, parts, UNIT, LANES), F32)
        out = pl.pallas_call(
            functools.partial(compact_kernel, (rows, width, STATIC, late)),
            out_shape=jax.ShapeDtypeStruct((rows, width), BF16),
            in_specs=[anywhere] * 8,
            out_specs=anywhere,
            scratch_shapes=[
                pltpu.SMEM((picks.size,), jnp.int32),
                pltpu.SMEM((shares.size,), F32),
                pltpu.SMEM((UNIT, LANES), jnp.int32),
                pltpu.VMEM((rows, width), BF16),
                pltpu.VMEM((rows, width), F32),
                *[pltpu.VMEM((rows + 1, parts, LANES), F32) for _ in range(2)],
                staged,
                pltpu.VMEM((TILE, width), BF16),
                pltpu.VMEM((TILE, parts, LANES), F32),
                *double,
                *[pltpu.SemaphoreType.DMA(shape) for shape in ((5,), (2, 3), (4,))],
            ],
            compiler_params=pltpu.CompilerParams(vmem_limit_bytes=62 * 1024 * 1024),
        )(picks, shares, counts, tokens, base, gate_all, up_all, down_all)
        return out.reshape(resid_in.shape)

    return jax.shard_map(local_program, mesh=mesh, in_specs=(tok_spec, tok_spec, tok_spec, rep_three, rep_three, rep_three, rep_three, rep_two, rep_two, rep_two, rep_two, rep_one, rep_one, rep_one, expert_spec, expert_spec, expert_spec), out_specs=tok_spec, check_vma=False)
```

```python
import functools
import math

import jax
import jax.numpy as jnp
import numpy as np
from jax import lax
from jax.experimental import pallas as pl
from jax.experimental.pallas import tpu as pltpu
from jax.sharding import PartitionSpec as P

EPS = 1e-6
ROPE_BASE = 10000.0
LANES = 128
F32 = jnp.float32
BF16 = jnp.bfloat16

UNIT = 8
TILE = 256
STATIC = 18

SIDE = 4
NEAR = (1, 3)
BLOCKS = (
    (0, 0), *[(a, 0) for a in NEAR], *[(0, a) for a in NEAR], *[(a, b) for a in NEAR for b in NEAR],
    *[place for a in (0, *NEAR) for place in ((2, a), (a, 2))], (2, 2))
STEPS = ((1, 0), (-1, 0), (0, 1), (0, -1))
GATE, UP, LOW, HIGH, LOW_A, LOW_B, HIGH_A, HIGH_B = range(8)
X_FIRST, Y_FIRST = (GATE, LOW), (UP, HIGH)
ALL = (*X_FIRST, *Y_FIRST)
LAST = ((1, 2), (3, 2), (2, 1), (2, 3))


def block_of(dx, dy):
    return BLOCKS.index((dx % SIDE, dy % SIDE))


def send_plan():
    plan = [[] for _ in range(5)]
    used = [0] * len(STEPS)

    def send(service, link, pieces, dx, dy):
        sx, sy = STEPS[link]
        for piece in pieces:
            plan[service].append((link, used[link], piece, block_of(dx, dy), block_of(dx + sx, dy + sy)))
            used[link] += 1

    def spread(service, dx, dy):
        pieces, start = (X_FIRST, 2) if dy == 0 else (Y_FIRST, 0)
        send(service, start, pieces, dx, dy)
        send(service, start + 1, pieces[::-1], dx, dy)

    def relay(service, pieces, blocks):
        for link, (piece, block) in enumerate(zip(pieces, blocks)):
            send(service, link, (piece,), *block)

    for link, order in enumerate((X_FIRST, X_FIRST[::-1], Y_FIRST, Y_FIRST[::-1])):
        send(0, link, order, 0, 0)
    for link, order in enumerate((Y_FIRST, Y_FIRST[::-1], X_FIRST, X_FIRST[::-1])):
        send(0, link, order, 0, 0)

    relay(1, (GATE, LOW, UP, HIGH), BLOCKS[1:5])
    for a in NEAR:
        spread(1, 0, a)
        spread(1, a, 0)
    relay(2, (HIGH, UP, LOW, GATE), BLOCKS[1:5])
    spread(2, 0, 2)
    spread(2, 2, 0)
    for a in NEAR:
        relay(3, (UP, HIGH, GATE, LOW), ((1, a), (3, a), (a, 1), (a, 3)))
    relay(4, (HIGH_A, UP, LOW_A, GATE), LAST)
    for link, piece in ((1, HIGH_B), (3, LOW_B)):
        send(4, link, (piece,), *LAST[link])
    return plan


def wait_plan():
    rows, cols = [(a, 0) for a in NEAR], [(0, a) for a in NEAR]
    far_rows, far_cols = [(2, a) for a in NEAR], [(a, 2) for a in NEAR]

    def need(first, second):
        return [(block, X_FIRST) for block in first] + [(block, Y_FIRST) for block in second]

    return [
        [],
        need(rows, cols),
        need(cols + [(2, 0)], rows + [(0, 2)]),
        [((a, b), ALL) for a in NEAR for b in NEAR],
        need([(0, 2)] + far_rows, [(2, 0)] + far_cols),
        [((2, 1), Y_FIRST), ((1, 2), X_FIRST), ((2, 3), (HIGH,)), ((3, 2), (LOW,))],
        [((2, 3), (UP,)), ((3, 2), (GATE,)), ((2, 2), (UP, GATE, HIGH_A, LOW_A, HIGH_B, LOW_B))],
    ]


def matmul(left, right):
    return jnp.dot(left, right, preferred_element_type=F32)


def matmul_t(left, right):
    return lax.dot_general(left, right, (((1,), (1,)), ((), ())), preferred_element_type=F32)


def norm_scale_of(values):
    return lax.rsqrt(jnp.mean(values * values, axis=-1, keepdims=True) + EPS)


def fused_kernel(
    dims,
    x_hbm, ids_hbm, router_hbm, na_hbm, nf_hbm, nm_hbm, rope_hbm, wq_hbm, wk_hbm, wv_hbm, wo_hbm, fg_hbm, fu_hbm, fd_hbm, eg_hbm, eu_hbm, ed_hbm,
    base_hbm, tokens_hbm, picks_hbm, shares_hbm, counts_hbm, gg_hbm, gu_hbm, gd_hbm,
    picks, shares, lots, counts, xs, acc, gates, qs, ks, vs, os, s_outer, s_inner, p_outer, p_inner, tops, sums, ids, router, na, nf, nm, rope, wqkv, wo, wg, wu, wd,
    load_sem, w_sem, out_sem, ici_send, ici_recv, d2d_send, d2d_recv,
):
    rows, width, seq, hidden, heads, kv_heads, head = dims
    micro = rows // seq
    half = hidden // 2
    experts = 2 * len(BLOCKS)
    ffn_steps = fg_hbm.shape[1] // hidden
    steps = ffn_steps + STATIC
    late = experts - STATIC
    me = lax.axis_index('ep')
    core = lax.rem(me, 2)
    col = lax.rem(me // 2, SIDE)
    row = me // (2 * SIDE)

    def device(dx, dy, flip):
        cx = lax.rem(col + dx + SIDE, SIDE)
        cy = lax.rem(row + dy + SIDE, SIDE)
        return {'ep': (cy * SIDE + cx) * 2 + lax.rem(core + flip, 2)}

    def cut(piece, gate, up, down):
        if piece < LOW:
            return (gate, up)[piece]
        start, size = {LOW: (0, 2), HIGH: (2, 2), LOW_A: (0, 1), LOW_B: (1, 1), HIGH_A: (2, 1), HIGH_B: (3, 1)}[piece]
        return down.at[pl.ds(start * hidden // 4, size * hidden // 4)]

    def piece_ref(block, piece):
        if block == 0:
            return cut(piece, eg_hbm.at[0], eu_hbm.at[0], ed_hbm.at[0])
        return slot_ref(2 * block, piece)

    def slot_ref(slot, piece):
        return cut(piece, gg_hbm.at[slot], gu_hbm.at[slot], gd_hbm.at[slot])

    def ici_copy(link, place, piece, source, target):
        return pltpu.make_async_remote_copy(
            src_ref=piece_ref(source, piece), dst_ref=slot_ref(2 * target, piece),
            send_sem=ici_send.at[link, place], recv_sem=ici_recv.at[target, piece],
            device_id=device(*STEPS[link], 0), device_id_type=pl.DeviceIdType.MESH)

    def d2d_copy(block, piece, source):
        return pltpu.make_async_remote_copy(
            src_ref=source, dst_ref=slot_ref(2 * block + 1, piece), send_sem=d2d_send.at[block, piece], recv_sem=d2d_recv.at[block, piece],
            device_id=device(0, 0, 1), device_id_type=pl.DeviceIdType.MESH)

    def pieces_of(block):
        return waits[-1][-1][1] if block == len(BLOCKS) - 1 else ALL

    def d2d_wait(block, pieces=ALL):
        for piece in pieces:
            d2d_copy(block, piece, slot_ref(2 * block + 1, piece)).wait_recv()

    plan = send_plan()
    waits = wait_plan()
    arrival = {(target, piece): (link, place, piece, source, target) for stage in plan for link, place, piece, source, target in stage}

    def service(point):
        landed = [(block_of(*block), piece) for block, pieces in waits[point] for piece in pieces]
        for block, piece in landed:
            ici_copy(*arrival[block, piece]).wait_recv()
            if point >= len(plan):
                d2d_copy(block, piece, piece_ref(block, piece)).start()
        if point < len(plan):
            for entry in plan[point]:
                ici_copy(*entry).start()
            for block, piece in landed if point else [(0, piece) for piece in ALL]:
                d2d_copy(block, piece, piece_ref(block, piece)).start()

    loads = [
        (x_hbm, xs.at[1]), (na_hbm, na), (nf_hbm, nf), (nm_hbm, nm), (router_hbm, router), (ids_hbm, ids), (rope_hbm, rope),
        (wq_hbm.at[pl.ds(0, 512)], wqkv.at[0]), (wq_hbm.at[pl.ds(512, 512)], wqkv.at[1]), (wk_hbm, wqkv.at[2]), (wv_hbm, wqkv.at[3]),
        (wo_hbm.at[pl.ds(0, 512)], wo.at[0]), (wo_hbm.at[pl.ds(512, 512)], wo.at[1]),
    ]
    loads = [pltpu.make_async_copy(source, target, load_sem.at[k]) for k, (source, target) in enumerate(loads)]
    for copy in loads:
        copy.start()

    barrier = pltpu.get_barrier_semaphore()
    for peer in [device(*step, 0) for step in STEPS] + [device(0, 0, 1)]:
        pl.semaphore_signal(barrier, inc=1, device_id=peer, device_id_type=pl.DeviceIdType.MESH)
    pl.semaphore_wait(barrier, len(STEPS) + 1)
    service(0)

    def expert_copies(slot, sources):
        return [pltpu.make_async_copy(source, buffer.at[slot], w_sem.at[slot, k]) for k, (source, buffer) in enumerate(zip(sources, (wg, wu, wd)))]

    def prefetch(step, slot):
        @pl.when(step < ffn_steps)
        def _():
            cut = pl.ds(pl.multiple_of(step * hidden, hidden), hidden)
            for copy in expert_copies(slot, (fg_hbm.at[:, cut], fu_hbm.at[:, cut], fd_hbm.at[cut])):
                copy.start()

        @pl.when(step == ffn_steps)
        def _():
            for copy in expert_copies(slot, (eg_hbm.at[0], eu_hbm.at[0], ed_hbm.at[0])):
                copy.start()

        @pl.when((step > ffn_steps) & (step < steps))
        def _():
            rank = step - ffn_steps

            @pl.when(lax.rem(rank, 2) == 1)
            def _():
                d2d_wait(rank // 2)

            for copy in expert_copies(slot, (gg_hbm.at[rank], gu_hbm.at[rank], gd_hbm.at[rank])):
                copy.start()

    prefetch(0, 0)

    for copy in loads[:6]:
        copy.wait()
    norm_attn, norm_ffn, norm_moe = [scale[...].astype(F32).reshape(1, width) for scale in (na, nf, nm)]
    ranks = lax.broadcasted_iota(jnp.int32, (experts, 1), 0)
    owner = jnp.zeros((experts, 1), jnp.int32)
    for block, (dx, dy) in enumerate(BLOCKS):
        chip = lax.rem(row - dy + SIDE, SIDE) * SIDE + lax.rem(col - dx + SIDE, SIDE)
        owner = jnp.where(ranks // 2 == block, chip, owner)
    owner = owner * 2 + lax.rem(core + lax.rem(ranks, 2), 2)
    ordered = (lax.broadcasted_iota(jnp.int32, (experts, experts), 1) == owner).astype(F32).astype(BF16)
    ordered = matmul(ordered, router[...]).astype(BF16)
    tile = 512
    tile_lanes = lax.broadcasted_iota(jnp.int32, (tile, LANES), 1)
    spots = lax.broadcasted_iota(jnp.int32, (tile, tile), 1)
    earlier = (lax.broadcasted_iota(jnp.int32, (tile, tile), 0) > spots).astype(F32).astype(BF16)
    spots = spots.astype(F32)
    quarters = tile // LANES
    list_lines = (rows // 2 + TILE) // LANES
    picks[...] = jnp.zeros_like(picks)
    shares[...] = jnp.zeros_like(shares)

    def prologue(halves, index, so_far):
        part = pl.ds(pl.multiple_of(index * tile, tile), tile)
        values = xs[1, part, :].astype(F32)
        unit = values * norm_scale_of(values)
        tokens = (unit * norm_moe).astype(BF16)
        xs[0, part, :] = (unit * norm_attn).astype(BF16)
        xs[1, part, :] = tokens
        acc[part, :] = values
        logits = matmul_t(ordered, tokens)
        per_seq = seq // tile
        wanted = ids[index // per_seq, :, pl.ds(pl.multiple_of(lax.rem(index, per_seq) * tile, tile), tile)]
        picked = wanted[0:1, :] == owner
        for choice in range(1, wanted.shape[0]):
            picked = picked | (wanted[choice:choice + 1, :] == owner)
        top = jnp.max(jnp.where(picked, logits, -jnp.inf), axis=0, keepdims=True)
        powers = jnp.where(picked, jnp.exp(jnp.where(picked, logits, top) - top), 0.0)
        share = powers / jnp.sum(powers, axis=0, keepdims=True)
        lots[...] = share
        share = jnp.concatenate([share, jnp.zeros((LANES - experts, tile), F32)], axis=0)
        share = share.T
        gates[part, :] = share

        chosen = share > 0.0
        ones = chosen.astype(F32)
        place = jnp.where(chosen, matmul(earlier, ones.astype(BF16)) + so_far, -1.0)
        so_far = so_far + jnp.sum(ones, axis=0, keepdims=True)
        token = lax.broadcasted_iota(jnp.int32, (1, tile), 1) + (index * tile + 1)
        major, minor = (token // TILE).astype(F32), lax.rem(token, TILE).astype(F32)

        def listed(rank, inner):
            spot = jnp.sum(jnp.where(tile_lanes == rank + STATIC, place, 0.0), axis=1, keepdims=True)
            weight = lots[pl.ds(rank + STATIC, 1), :]
            high = weight.astype(BF16).astype(F32)
            middle = (weight - high).astype(BF16).astype(F32)
            facts = jnp.concatenate([major, minor, high, middle, weight - high - middle, jnp.zeros((3, tile), F32)], axis=0).astype(BF16)
            for half in range(halves):
                found = matmul(facts, jnp.where(spot - half * tile == spots, 1.0, 0.0).astype(BF16))
                row = (found[0:1] * TILE + found[1:2]).astype(jnp.int32)
                share_row = found[2:3] + found[3:4] + found[4:5]
                for lane_cut in range(quarters):
                    line = pl.ds(rank * list_lines + half * quarters + lane_cut, 1)
                    lane_span = slice(lane_cut * LANES, (lane_cut + 1) * LANES)
                    picks[line, :] += row[:, lane_span]
                    shares[line, :] += share_row[:, lane_span]
            return inner

        lax.fori_loop(0, late, listed, 0)
        return so_far

    taken = jnp.zeros((1, LANES), F32)
    for micro_index in range(micro):
        first_tile = micro_index * seq // tile
        taken = lax.fori_loop(first_tile, first_tile + seq // tile, functools.partial(prologue, micro_index + 1), taken)
    counts[...] = jnp.broadcast_to(taken, counts.shape).astype(jnp.int32)
    results = [(xs.at[1], tokens_hbm), (picks, picks_hbm), (shares, shares_hbm), (counts, counts_hbm), (acc, base_hbm)]
    results = [pltpu.make_async_copy(source, target, out_sem.at[k]) for k, (source, target) in enumerate(results)]
    for copy in results[:-1]:
        copy.start()
    for copy in loads[6:]:
        copy.wait()

    def sequence(micro_index, carry):
        base = pl.multiple_of(micro_index * seq, seq)

        @pl.when(micro_index == 1)
        def _():
            service(1)

        lane = lax.broadcasted_iota(jnp.int32, (seq, LANES), 1)
        first = lax.rem(lane, head) < head // 2
        low = lane < head
        cosine, sine = rope[0], rope[1]
        tokens = xs[0, pl.ds(base, seq), :]

        def rotated(values):
            swapped = jnp.where(first, pltpu.roll(values, LANES - head // 2, 1), pltpu.roll(values, head // 2, 1))
            return values * cosine + swapped * sine

        def doubled(values, target, pair):
            turned = pltpu.roll(values, head, 1)
            place = 2 * pair * LANES
            target[:, place:place + LANES] = jnp.where(low, values, turned).astype(BF16)
            target[:, place + LANES:place + 2 * LANES] = jnp.where(low, turned, values).astype(BF16)

        for block in range(4):
            flat = matmul_t(tokens, wqkv[block])
            for piece in range(512 // LANES):
                values = flat[:, piece * LANES:(piece + 1) * LANES]
                if block < 2:
                    place = block * 512 + piece * LANES
                    qs[:, place:place + LANES] = (rotated(values) * head ** -0.5).astype(BF16)
                elif block == 2:
                    doubled(rotated(values), ks, piece)
                else:
                    doubled(values, vs, piece)

        chunk = 256
        chunk_low = lax.broadcasted_iota(jnp.int32, (chunk, LANES), 1) < head
        inside = lax.rem(lax.broadcasted_iota(jnp.int32, (2 * chunk, chunk), 0), chunk) >= lax.broadcasted_iota(jnp.int32, (2 * chunk, chunk), 1)

        def columns(index):
            return pl.ds(pl.multiple_of(index * LANES, LANES), LANES)

        def score(index, parts, target):
            cols, place = columns(index), 0
            for part in parts:
                span = (part + 1) * chunk
                q_part = qs[part * chunk:span, cols]
                none = jnp.zeros_like(q_part)
                pair = jnp.concatenate([jnp.where(chunk_low, q_part, none), jnp.where(chunk_low, none, q_part)], axis=0)
                scores = matmul_t(pair, ks[:span, cols])
                edge = jnp.where(inside, scores[:, part * chunk:], -1e30)
                scores = edge if part == 0 else jnp.concatenate([scores[:, :part * chunk], edge], axis=1)
                target[:, place:place + span] = scores
                tops[part] = jnp.broadcast_to(jnp.max(scores, axis=1, keepdims=True), tops.shape[1:])
                place += span

        def soften(parts, origin, target):
            place = 0
            for part in parts:
                top = tops[part]
                total = jnp.zeros_like(top)
                for _ in range((part + 1) * chunk // LANES):
                    powers = jnp.exp(origin[:, place:place + LANES] - top)
                    total = total + powers
                    target[:, place:place + LANES] = powers.astype(BF16)
                    place += LANES
                sums[part] = jnp.broadcast_to(jnp.sum(total, axis=1, keepdims=True), sums.shape[1:])

        def mix(index, parts, origin):
            cols, place = columns(index), 0
            for part in parts:
                span = (part + 1) * chunk
                mixed = matmul(origin[:, place:place + span], vs[:span, cols]) / sums[part]
                os[part * chunk:span, cols] = jnp.where(chunk_low, mixed[:chunk], mixed[chunk:]).astype(BF16)
                place += span

        outer_parts, inner_parts = (0, 3), (1, 2)
        score(0, outer_parts, s_outer)

        def group(index, inner):
            score(index, inner_parts, s_inner)
            soften(outer_parts, s_outer, p_outer)
            mix(lax.rem(index + kv_heads - 1, kv_heads), inner_parts, p_inner)
            score(lax.rem(index + 1, kv_heads), outer_parts, s_outer)
            soften(inner_parts, s_inner, p_inner)
            mix(index, outer_parts, p_outer)
            return inner

        lax.fori_loop(0, kv_heads, group, 0)
        mix(kv_heads - 1, inner_parts, p_inner)

        def project(index, inner):
            local = pl.ds(pl.multiple_of(index * tile, tile), tile)
            part = pl.ds(pl.multiple_of(base + index * tile, tile), tile)
            added = matmul(os[local, :tile], wo[0]) + matmul(os[local, tile:], wo[1])
            after = (acc[part, :] + added).astype(BF16).astype(F32)
            acc[part, :] = after
            xs[0, part, :] = (after * norm_scale_of(after) * norm_ffn).astype(BF16)
            return inner

        lax.fori_loop(0, seq // tile, project, 0)
        return carry

    lax.fori_loop(0, micro, sequence, 0)

    big = 1024
    lanes = lax.broadcasted_iota(jnp.int32, (big, LANES), 1)
    moments = {5: 2, 14: 3, 21: 4, 24: 5}

    def ffn_step(dense, step, carry):
        slot = lax.rem(step, 2)
        for copy in expert_copies(slot, (gg_hbm.at[0], gu_hbm.at[0], gd_hbm.at[0])):
            copy.wait()
        for moment, point in moments.items():
            if dense == (moment < ffn_steps):
                @pl.when(step == moment)
                def _():
                    service(point)

        prefetch(step + 1, 1 - slot)
        gate_w, up_w, down_w = wg.at[slot], wu.at[slot], wd.at[slot]

        def rows_step(index, inner):
            part = pl.ds(pl.multiple_of(index * big, big), big)
            tokens = xs[0 if dense else 1, part, :]
            mixed = jax.nn.silu(matmul(tokens, gate_w[...])) * matmul(tokens, up_w[...])
            if dense:
                acc[part, :] += matmul(mixed.astype(BF16), down_w[...])
            else:
                weight = jnp.sum(jnp.where(lanes == step - ffn_steps, gates[part, :], 0.0), axis=1, keepdims=True)
                mixed = jnp.where(weight > 0.0, mixed, 0.0).astype(BF16)
                acc[part, :] += weight * matmul(mixed, down_w[...]).astype(BF16).astype(F32)
            return inner

        lax.fori_loop(0, rows // big, rows_step, 0)
        return carry

    lax.fori_loop(0, ffn_steps, functools.partial(ffn_step, True), 0)
    lax.fori_loop(ffn_steps, steps, functools.partial(ffn_step, False), 0)

    results[-1].start()
    service(len(waits) - 1)
    for block in range(STATIC // 2, len(BLOCKS)):
        d2d_wait(block, pieces_of(block))
    for stage in plan:
        for entry in stage:
            ici_copy(*entry).wait_send()
    for block in range(len(BLOCKS)):
        for piece in pieces_of(block):
            d2d_copy(block, piece, piece_ref(block, piece)).wait_send()
    for copy in results:
        copy.wait()


def compact_kernel(
    dims,
    picks_hbm, shares_hbm, counts_hbm, tokens_hbm, base_hbm, gg_hbm, gu_hbm, gd_hbm,
    out_hbm,
    picks, shares, counts, tokens, base, table, total, packed, lhs, result, wg, wu, wd,
    load_sem, w_sem, out_sem,
):
    rows, width, first, ranks = dims
    list_size = rows // 2 + TILE
    parts = width // LANES
    experts = first + ranks
    loads = [pltpu.make_async_copy(source, target, load_sem.at[k]) for k, (source, target) in enumerate((
        (tokens_hbm, tokens), (picks_hbm, picks), (shares_hbm, shares), (counts_hbm, counts), (base_hbm, base)))]
    for copy in loads:
        copy.start()

    def weights(rank, slot):
        return [pltpu.make_async_copy(source.at[first + rank], buffer.at[slot], w_sem.at[slot, k])
                for k, (source, buffer) in enumerate(((gg_hbm, wg), (gu_hbm, wu), (gd_hbm, wd)))]

    for copy in weights(0, 0):
        copy.start()

    loads[0].wait()
    table[0] = jnp.zeros((parts, LANES), F32)
    total[0] = jnp.zeros((parts, LANES), F32)
    flat = table.reshape((rows + 1) * parts, LANES)
    step_rows = 512

    def spread(index, carry):
        start = pl.multiple_of(index * step_rows, step_rows)
        values = tokens[pl.ds(start, step_rows), :].astype(F32)
        for part in range(parts):
            flat[pl.ds(parts + start * parts + part, step_rows, stride=parts), :] = values[:, part * LANES:(part + 1) * LANES]
        total[pl.ds(1 + start, step_rows)] = jnp.zeros((step_rows, parts, LANES), F32)
        return carry

    lax.fori_loop(0, rows // step_rows, spread, 0)
    for copy in loads[1:4]:
        copy.wait()

    def tiles_of(rank):
        return jnp.maximum((counts[0, first + rank] + TILE - 1) // TILE, 1)

    def gather(rank, tile):
        start = rank * list_size + tile * TILE
        for place in range(TILE):
            spots = pl.ds(place // UNIT * UNIT * parts + place % UNIT, parts, stride=UNIT)
            packed.reshape(TILE * parts, LANES)[spots, :] = table[picks[start + place]]

    def scatter(rank, tile):
        start = rank * list_size + tile * TILE
        for group in range(0, TILE, UNIT):
            rows_of = [picks[start + group + place] for place in range(UNIT)]
            sums = [total[row] + result[group + place] for place, row in enumerate(rows_of)]
            for row, value in zip(rows_of, sums):
                total[row] = value

    def factor(rank, tile):
        line = (rank * list_size + tile * TILE) // LANES
        lines = [jnp.broadcast_to(shares[pl.ds(line + k, 1), :], (LANES, LANES)).T for k in range(TILE // LANES)]
        return jnp.concatenate(lines, axis=0)

    count = lax.fori_loop(0, ranks, lambda rank, so_far: so_far + tiles_of(rank), 0)
    gather(0, 0)

    def tile_step(index, carry):
        rank, tile, last_rank, last_tile = carry
        slot = lax.rem(rank, 2)

        @pl.when(tile == 0)
        def _():
            for copy in weights(rank, slot):
                copy.wait()

            @pl.when(rank + 1 < ranks)
            def _():
                for copy in weights(rank + 1, 1 - slot):
                    copy.start()

        more = tile + 1 < tiles_of(rank)
        next_rank = jnp.where(more, rank, rank + 1)
        next_tile = jnp.where(more, tile + 1, 0)
        for part in range(parts):
            lhs[:, part * LANES:(part + 1) * LANES] = packed[:, part].reshape(TILE, LANES).astype(BF16)
        scatter(last_rank, last_tile)
        gather(next_rank, next_tile)
        gate_act = matmul(lhs[...], wg[slot])
        up_act = matmul(lhs[...], wu[slot])
        mixed = (jax.nn.silu(gate_act) * up_act).astype(BF16)
        down = matmul(mixed, wd[slot]).astype(BF16).astype(F32)
        share = factor(rank, tile)
        for part in range(parts):
            result.reshape(TILE * parts, LANES)[pl.ds(part, TILE, stride=parts), :] = share * down[:, part * LANES:(part + 1) * LANES]
        return next_rank, next_tile, rank, tile

    _, _, last_rank, last_tile = lax.fori_loop(0, count, tile_step, (jnp.int32(0), jnp.int32(0), jnp.int32(ranks), jnp.int32(0)))
    scatter(last_rank, last_tile)
    loads[4].wait()
    sums_of = total.reshape((rows + 1) * parts, LANES)

    def store(index):
        part = pl.ds(index * step_rows, step_rows)
        return pltpu.make_async_copy(tokens.at[part], out_hbm.at[part], out_sem.at[index])

    for index in range(rows // step_rows):
        span = slice(index * step_rows, (index + 1) * step_rows)
        for part in range(parts):
            cols = slice(part * LANES, (part + 1) * LANES)
            moe = sums_of[pl.ds(parts + index * step_rows * parts + part, step_rows, stride=parts), :]
            tokens[span, cols] = (base[span, cols] + moe).astype(BF16)
        store(index).start()
    for index in range(rows // step_rows):
        store(index).wait()

def rope_tables(seq, head):
    half = head // 2
    freqs = np.float32(ROPE_BASE) ** (-np.arange(half, dtype=np.float32) * np.float32(2.0) / np.float32(head))
    angles = np.arange(seq, dtype=np.float32)[:, None] * freqs.astype(np.float32)[None, :]
    cosine = np.cos(angles.astype(np.float64)).astype(np.float32)
    sine = np.sin(angles.astype(np.float64)).astype(np.float32)
    times = LANES // head
    return np.stack([np.tile(np.concatenate([cosine, cosine], 1), (1, times)), np.tile(np.concatenate([-sine, sine], 1), (1, times))])


def solution(mesh):
    tok_spec = P(None, ('dp', 'ep'), None, None)
    rep_one = P(None)
    rep_two = P(None, None)
    rep_three = P(None, None, None)
    expert_spec = P('ep', None, None)
    assert mesh.shape['ep'] == 2 * SIDE * SIDE

    def local_program(resid_in, expert_idx, expert_slot, w_query, w_key, w_value, w_out, w_gate, w_up, w_down, w_router, norm_attn, norm_ffn, norm_moe, expert_gate, expert_up, expert_down):
        micro, seqs, seq, width = resid_in.shape
        choices = expert_idx.shape[-1]
        heads, head = w_query.shape[1:]
        kv_heads = w_key.shape[1]
        hidden = expert_gate.shape[2]
        experts = 2 * len(BLOCKS)
        rows = micro * seqs * seq
        ids = expert_idx.transpose(0, 1, 3, 2).reshape(micro * seqs, choices, seq)
        rope = jnp.asarray(rope_tables(seq, head))
        anywhere = pl.BlockSpec(memory_space=pl.ANY)
        operands = (
            resid_in.reshape(rows, width), ids, w_router.T, norm_attn, norm_ffn, norm_moe, rope,
            w_query.transpose(1, 2, 0).reshape(heads * head, width), w_key.transpose(1, 2, 0).reshape(kv_heads * head, width),
            w_value.transpose(1, 2, 0).reshape(kv_heads * head, width), w_out.reshape(heads * head, width),
            w_gate, w_up, w_down, expert_gate, expert_up, expert_down)
        flops = rows * width * 2 * (3 * hidden * experts + 3 * w_gate.shape[1] + 3 * heads * head)
        late = experts - STATIC
        list_size = rows // 2 + TILE
        lists = ((late + 1) * list_size // LANES, LANES)
        weight_shapes = ((width, hidden), (width, hidden), (hidden, width))
        double = [pltpu.VMEM((2,) + shape, BF16) for shape in weight_shapes]
        base, tokens, picks, shares, counts, gate_all, up_all, down_all = pl.pallas_call(
            functools.partial(fused_kernel, (rows, width, seq, hidden, heads, kv_heads, head)),
            out_shape=tuple(jax.ShapeDtypeStruct(shape, kind) for shape, kind in (
                ((rows, width), F32), ((rows, width), BF16), (lists, jnp.int32), (lists, F32), ((UNIT, LANES), jnp.int32),
                *[((experts,) + shape, BF16) for shape in weight_shapes])),
            in_specs=[anywhere] * len(operands),
            out_specs=[anywhere] * 8,
            scratch_shapes=[
                pltpu.VMEM(lists, jnp.int32),
                pltpu.VMEM(lists, F32),
                pltpu.VMEM((experts, 512), F32),
                pltpu.VMEM((UNIT, LANES), jnp.int32),
                pltpu.VMEM((2, rows, width), BF16),
                pltpu.VMEM((rows, width), F32),
                pltpu.VMEM((rows, LANES), F32),
                *[pltpu.VMEM((seq, heads * head), BF16) for _ in range(4)],
                *[pltpu.VMEM((512, 1280), kind) for kind in (F32, F32, BF16, BF16)],
                *[pltpu.VMEM((4, 512, LANES), F32) for _ in range(2)],
                pltpu.VMEM((micro * seqs, choices, seq), jnp.int32),
                pltpu.VMEM((experts, width), BF16),
                *[pltpu.VMEM((width,), BF16) for _ in range(3)],
                pltpu.VMEM((2, seq, LANES), F32),
                pltpu.VMEM((4, 512, width), BF16),
                pltpu.VMEM((2, 512, width), BF16),
                *double,
                *[pltpu.SemaphoreType.DMA(shape) for shape in ((13,), (2, 3), (5,), (4, 16), (16, 8), (16, 8), (16, 8))],
            ],
            compiler_params=pltpu.CompilerParams(collective_id=0, has_side_effects=True, vmem_limit_bytes=62 * 1024 * 1024),
            cost_estimate=pl.CostEstimate(flops=flops, bytes_accessed=experts * 6 * width * hidden, transcendentals=0),
        )(*operands)
        parts = width // LANES
        picks = picks.reshape(-1)
        staged = pltpu.VMEM((TILE // UNIT, parts, UNIT, LANES), F32)
        out = pl.pallas_call(
            functools.partial(compact_kernel, (rows, width, STATIC, late)),
            out_shape=jax.ShapeDtypeStruct((rows, width), BF16),
            in_specs=[anywhere] * 8,
            out_specs=anywhere,
            scratch_shapes=[
                pltpu.SMEM((picks.size,), jnp.int32),
                pltpu.VMEM(lists, F32),
                pltpu.SMEM((UNIT, LANES), jnp.int32),
                pltpu.VMEM((rows, width), BF16),
                pltpu.VMEM((rows, width), F32),
                *[pltpu.VMEM((rows + 1, parts, LANES), F32) for _ in range(2)],
                staged,
                pltpu.VMEM((TILE, width), BF16),
                pltpu.VMEM((TILE, parts, LANES), F32),
                *double,
                *[pltpu.SemaphoreType.DMA(shape) for shape in ((5,), (2, 3), (4,))],
            ],
            compiler_params=pltpu.CompilerParams(vmem_limit_bytes=62 * 1024 * 1024),
        )(picks, shares, counts, tokens, base, gate_all, up_all, down_all)
        return out.reshape(resid_in.shape)

    return jax.shard_map(local_program, mesh=mesh, in_specs=(tok_spec, tok_spec, tok_spec, rep_three, rep_three, rep_three, rep_three, rep_two, rep_two, rep_two, rep_two, rep_one, rep_one, rep_one, expert_spec, expert_spec, expert_spec), out_specs=tok_spec, check_vma=False)
```

```python
import functools
import math

import jax
import jax.numpy as jnp
import numpy as np
from jax import lax
from jax.experimental import pallas as pl
from jax.experimental.pallas import tpu as pltpu
from jax.sharding import PartitionSpec as P

EPS = 1e-6
ROPE_BASE = 10000.0
LANES = 128
F32 = jnp.float32
BF16 = jnp.bfloat16

UNIT = 8
TILE = 256
STATIC = 18

SIDE = 4
NEAR = (1, 3)
BLOCKS = (
    (0, 0), *[(a, 0) for a in NEAR], *[(0, a) for a in NEAR], *[(a, b) for a in NEAR for b in NEAR],
    *[place for a in (0, *NEAR) for place in ((2, a), (a, 2))], (2, 2))
STEPS = ((1, 0), (-1, 0), (0, 1), (0, -1))
GATE, UP, LOW, HIGH, LOW_A, LOW_B, HIGH_A, HIGH_B = range(8)
X_FIRST, Y_FIRST = (GATE, LOW), (UP, HIGH)
ALL = (*X_FIRST, *Y_FIRST)
LAST = ((1, 2), (3, 2), (2, 1), (2, 3))


def block_of(dx, dy):
    return BLOCKS.index((dx % SIDE, dy % SIDE))


def send_plan():
    plan = [[] for _ in range(5)]
    used = [0] * len(STEPS)

    def send(service, link, pieces, dx, dy):
        sx, sy = STEPS[link]
        for piece in pieces:
            plan[service].append((link, used[link], piece, block_of(dx, dy), block_of(dx + sx, dy + sy)))
            used[link] += 1

    def spread(service, dx, dy):
        pieces, start = (X_FIRST, 2) if dy == 0 else (Y_FIRST, 0)
        send(service, start, pieces, dx, dy)
        send(service, start + 1, pieces[::-1], dx, dy)

    def relay(service, pieces, blocks):
        for link, (piece, block) in enumerate(zip(pieces, blocks)):
            send(service, link, (piece,), *block)

    for link, order in enumerate((X_FIRST, X_FIRST[::-1], Y_FIRST, Y_FIRST[::-1])):
        send(0, link, order, 0, 0)
    for link, order in enumerate((Y_FIRST, Y_FIRST[::-1], X_FIRST, X_FIRST[::-1])):
        send(0, link, order, 0, 0)

    relay(1, (GATE, LOW, UP, HIGH), BLOCKS[1:5])
    for a in NEAR:
        spread(1, 0, a)
        spread(1, a, 0)
    relay(2, (HIGH, UP, LOW, GATE), BLOCKS[1:5])
    spread(2, 0, 2)
    spread(2, 2, 0)
    for a in NEAR:
        relay(3, (UP, HIGH, GATE, LOW), ((1, a), (3, a), (a, 1), (a, 3)))
    relay(4, (HIGH_A, UP, LOW_A, GATE), LAST)
    for link, piece in ((1, HIGH_B), (3, LOW_B)):
        send(4, link, (piece,), *LAST[link])
    return plan


def wait_plan():
    rows, cols = [(a, 0) for a in NEAR], [(0, a) for a in NEAR]
    far_rows, far_cols = [(2, a) for a in NEAR], [(a, 2) for a in NEAR]

    def need(first, second):
        return [(block, X_FIRST) for block in first] + [(block, Y_FIRST) for block in second]

    return [
        [],
        need(rows, cols),
        need(cols + [(2, 0)], rows + [(0, 2)]),
        [((a, b), ALL) for a in NEAR for b in NEAR],
        need([(0, 2)] + far_rows, [(2, 0)] + far_cols),
        [((2, 1), Y_FIRST), ((1, 2), X_FIRST), ((2, 3), (HIGH,)), ((3, 2), (LOW,))],
        [((2, 3), (UP,)), ((3, 2), (GATE,)), ((2, 2), (UP, GATE, HIGH_A, LOW_A, HIGH_B, LOW_B))],
    ]


def matmul(left, right):
    return jnp.dot(left, right, preferred_element_type=F32)


def matmul_t(left, right):
    return lax.dot_general(left, right, (((1,), (1,)), ((), ())), preferred_element_type=F32)


def norm_scale_of(values):
    return lax.rsqrt(jnp.mean(values * values, axis=-1, keepdims=True) + EPS)


def fused_kernel(
    dims,
    x_hbm, ids_hbm, router_hbm, na_hbm, nf_hbm, nm_hbm, rope_hbm, wq_hbm, wk_hbm, wv_hbm, wo_hbm, fg_hbm, fu_hbm, fd_hbm, eg_hbm, eu_hbm, ed_hbm,
    base_hbm, tokens_hbm, picks_hbm, shares_hbm, counts_hbm, gg_hbm, gu_hbm, gd_hbm,
    picks, shares, lots, counts, xs, acc, gates, qs, ks, vs, os, s_outer, s_inner, p_outer, p_inner, tops, sums, ids, router, na, nf, nm, rope, wqkv, wo, wg, wu, wd,
    load_sem, w_sem, out_sem, ici_send, ici_recv, d2d_send, d2d_recv,
):
    rows, width, seq, hidden, heads, kv_heads, head = dims
    micro = rows // seq
    half = hidden // 2
    experts = 2 * len(BLOCKS)
    ffn_steps = fg_hbm.shape[1] // hidden
    steps = ffn_steps + STATIC
    late = experts - STATIC
    me = lax.axis_index('ep')
    core = lax.rem(me, 2)
    col = lax.rem(me // 2, SIDE)
    row = me // (2 * SIDE)

    def device(dx, dy, flip):
        cx = lax.rem(col + dx + SIDE, SIDE)
        cy = lax.rem(row + dy + SIDE, SIDE)
        return {'ep': (cy * SIDE + cx) * 2 + lax.rem(core + flip, 2)}

    def cut(piece, gate, up, down):
        if piece < LOW:
            return (gate, up)[piece]
        start, size = {LOW: (0, 2), HIGH: (2, 2), LOW_A: (0, 1), LOW_B: (1, 1), HIGH_A: (2, 1), HIGH_B: (3, 1)}[piece]
        return down.at[pl.ds(start * hidden // 4, size * hidden // 4)]

    def piece_ref(block, piece):
        if block == 0:
            return cut(piece, eg_hbm.at[0], eu_hbm.at[0], ed_hbm.at[0])
        return slot_ref(2 * block, piece)

    def slot_ref(slot, piece):
        return cut(piece, gg_hbm.at[slot], gu_hbm.at[slot], gd_hbm.at[slot])

    def ici_copy(link, place, piece, source, target):
        return pltpu.make_async_remote_copy(
            src_ref=piece_ref(source, piece), dst_ref=slot_ref(2 * target, piece),
            send_sem=ici_send.at[link, place], recv_sem=ici_recv.at[target, piece],
            device_id=device(*STEPS[link], 0), device_id_type=pl.DeviceIdType.MESH)

    def d2d_copy(block, piece, source):
        return pltpu.make_async_remote_copy(
            src_ref=source, dst_ref=slot_ref(2 * block + 1, piece), send_sem=d2d_send.at[block, piece], recv_sem=d2d_recv.at[block, piece],
            device_id=device(0, 0, 1), device_id_type=pl.DeviceIdType.MESH)

    def pieces_of(block):
        return waits[-1][-1][1] if block == len(BLOCKS) - 1 else ALL

    def d2d_wait(block, pieces=ALL):
        for piece in pieces:
            d2d_copy(block, piece, slot_ref(2 * block + 1, piece)).wait_recv()

    plan = send_plan()
    waits = wait_plan()
    arrival = {(target, piece): (link, place, piece, source, target) for stage in plan for link, place, piece, source, target in stage}

    def service(point):
        landed = [(block_of(*block), piece) for block, pieces in waits[point] for piece in pieces]
        for block, piece in landed:
            ici_copy(*arrival[block, piece]).wait_recv()
            if point >= len(plan):
                d2d_copy(block, piece, piece_ref(block, piece)).start()
        if point < len(plan):
            for entry in plan[point]:
                ici_copy(*entry).start()
            for block, piece in landed if point else [(0, piece) for piece in ALL]:
                d2d_copy(block, piece, piece_ref(block, piece)).start()

    loads = [
        (x_hbm, xs.at[1]), (na_hbm, na), (nf_hbm, nf), (nm_hbm, nm), (router_hbm, router), (ids_hbm, ids), (rope_hbm, rope),
        (wq_hbm.at[pl.ds(0, 512)], wqkv.at[0]), (wq_hbm.at[pl.ds(512, 512)], wqkv.at[1]), (wk_hbm, wqkv.at[2]), (wv_hbm, wqkv.at[3]),
        (wo_hbm.at[pl.ds(0, 512)], wo.at[0]), (wo_hbm.at[pl.ds(512, 512)], wo.at[1]),
    ]
    loads = [pltpu.make_async_copy(source, target, load_sem.at[k]) for k, (source, target) in enumerate(loads)]
    for copy in loads:
        copy.start()

    barrier = pltpu.get_barrier_semaphore()
    for peer in [device(*step, 0) for step in STEPS] + [device(0, 0, 1)]:
        pl.semaphore_signal(barrier, inc=1, device_id=peer, device_id_type=pl.DeviceIdType.MESH)
    pl.semaphore_wait(barrier, len(STEPS) + 1)
    service(0)

    def expert_copies(slot, sources):
        return [pltpu.make_async_copy(source, buffer.at[slot], w_sem.at[slot, k]) for k, (source, buffer) in enumerate(zip(sources, (wg, wu, wd)))]

    def prefetch(step, slot):
        @pl.when(step < ffn_steps)
        def _():
            cut = pl.ds(pl.multiple_of(step * hidden, hidden), hidden)
            for copy in expert_copies(slot, (fg_hbm.at[:, cut], fu_hbm.at[:, cut], fd_hbm.at[cut])):
                copy.start()

        @pl.when(step == ffn_steps)
        def _():
            for copy in expert_copies(slot, (eg_hbm.at[0], eu_hbm.at[0], ed_hbm.at[0])):
                copy.start()

        @pl.when((step > ffn_steps) & (step < steps))
        def _():
            rank = step - ffn_steps

            @pl.when(lax.rem(rank, 2) == 1)
            def _():
                d2d_wait(rank // 2)

            for copy in expert_copies(slot, (gg_hbm.at[rank], gu_hbm.at[rank], gd_hbm.at[rank])):
                copy.start()

    prefetch(0, 0)

    for copy in loads[:6]:
        copy.wait()
    norm_attn, norm_ffn, norm_moe = [scale[...].astype(F32).reshape(1, width) for scale in (na, nf, nm)]
    ranks = lax.broadcasted_iota(jnp.int32, (experts, 1), 0)
    owner = jnp.zeros((experts, 1), jnp.int32)
    for block, (dx, dy) in enumerate(BLOCKS):
        chip = lax.rem(row - dy + SIDE, SIDE) * SIDE + lax.rem(col - dx + SIDE, SIDE)
        owner = jnp.where(ranks // 2 == block, chip, owner)
    owner = owner * 2 + lax.rem(core + lax.rem(ranks, 2), 2)
    ordered = (lax.broadcasted_iota(jnp.int32, (experts, experts), 1) == owner).astype(F32).astype(BF16)
    ordered = matmul(ordered, router[...]).astype(BF16)
    tile = 512
    tile_lanes = lax.broadcasted_iota(jnp.int32, (tile, LANES), 1)
    spots = lax.broadcasted_iota(jnp.int32, (tile, tile), 1)
    earlier = (lax.broadcasted_iota(jnp.int32, (tile, tile), 0) > spots).astype(F32).astype(BF16)
    spots = spots.astype(F32)
    quarters = tile // LANES
    list_lines = (rows // 2 + TILE) // LANES
    picks[...] = jnp.zeros_like(picks)
    shares[...] = jnp.zeros_like(shares)

    def prologue(halves, index, so_far):
        part = pl.ds(pl.multiple_of(index * tile, tile), tile)
        values = xs[1, part, :].astype(F32)
        unit = values * norm_scale_of(values)
        tokens = (unit * norm_moe).astype(BF16)
        xs[0, part, :] = (unit * norm_attn).astype(BF16)
        xs[1, part, :] = tokens
        acc[part, :] = values
        logits = matmul_t(ordered, tokens)
        per_seq = seq // tile
        wanted = ids[index // per_seq, :, pl.ds(pl.multiple_of(lax.rem(index, per_seq) * tile, tile), tile)]
        picked = wanted[0:1, :] == owner
        for choice in range(1, wanted.shape[0]):
            picked = picked | (wanted[choice:choice + 1, :] == owner)
        top = jnp.max(jnp.where(picked, logits, -jnp.inf), axis=0, keepdims=True)
        powers = jnp.where(picked, jnp.exp(jnp.where(picked, logits, top) - top), 0.0)
        share = powers / jnp.sum(powers, axis=0, keepdims=True)
        lots[...] = share
        share = jnp.concatenate([share, jnp.zeros((LANES - experts, tile), F32)], axis=0)
        share = share.T
        gates[part, :] = share

        chosen = share > 0.0
        ones = chosen.astype(F32)
        place = jnp.where(chosen, matmul(earlier, ones.astype(BF16)) + so_far, -1.0)
        so_far = so_far + jnp.sum(ones, axis=0, keepdims=True)
        token = lax.broadcasted_iota(jnp.int32, (1, tile), 1) + (index * tile + 1)
        major, minor = (token // TILE).astype(F32), lax.rem(token, TILE).astype(F32)

        def listed(rank, inner):
            spot = jnp.sum(jnp.where(tile_lanes == rank + STATIC, place, 0.0), axis=1, keepdims=True)
            weight = lots[pl.ds(rank + STATIC, 1), :]
            high = weight.astype(BF16).astype(F32)
            middle = (weight - high).astype(BF16).astype(F32)
            facts = jnp.concatenate([major, minor, high, middle, weight - high - middle, jnp.zeros((3, tile), F32)], axis=0).astype(BF16)
            for half in range(halves):
                found = matmul(facts, jnp.where(spot - half * tile == spots, 1.0, 0.0).astype(BF16))
                row = (found[0:1] * TILE + found[1:2]).astype(jnp.int32)
                share_row = found[2:3] + found[3:4] + found[4:5]
                for lane_cut in range(quarters):
                    line = pl.ds(rank * list_lines + half * quarters + lane_cut, 1)
                    lane_span = slice(lane_cut * LANES, (lane_cut + 1) * LANES)
                    picks[line, :] += row[:, lane_span]
                    shares[line, :] += share_row[:, lane_span]
            return inner

        lax.fori_loop(0, late, listed, 0)
        return so_far

    taken = jnp.zeros((1, LANES), F32)
    for micro_index in range(micro):
        first_tile = micro_index * seq // tile
        taken = lax.fori_loop(first_tile, first_tile + seq // tile, functools.partial(prologue, micro_index + 1), taken)
    counts[...] = jnp.broadcast_to(taken, counts.shape).astype(jnp.int32)
    results = [(xs.at[1], tokens_hbm), (picks, picks_hbm), (shares, shares_hbm), (counts, counts_hbm), (acc, base_hbm)]
    results = [pltpu.make_async_copy(source, target, out_sem.at[k]) for k, (source, target) in enumerate(results)]
    for copy in results[:-1]:
        copy.start()
    for copy in loads[6:]:
        copy.wait()

    def sequence(micro_index, carry):
        base = pl.multiple_of(micro_index * seq, seq)

        @pl.when(micro_index == 1)
        def _():
            service(1)

        lane = lax.broadcasted_iota(jnp.int32, (seq, LANES), 1)
        first = lax.rem(lane, head) < head // 2
        low = lane < head
        cosine, sine = rope[0], rope[1]
        tokens = xs[0, pl.ds(base, seq), :]

        def rotated(values):
            swapped = jnp.where(first, pltpu.roll(values, LANES - head // 2, 1), pltpu.roll(values, head // 2, 1))
            return values * cosine + swapped * sine

        def doubled(values, target, pair):
            turned = pltpu.roll(values, head, 1)
            place = 2 * pair * LANES
            target[:, place:place + LANES] = jnp.where(low, values, turned).astype(BF16)
            target[:, place + LANES:place + 2 * LANES] = jnp.where(low, turned, values).astype(BF16)

        for block in range(4):
            flat = matmul_t(tokens, wqkv[block])
            for piece in range(512 // LANES):
                values = flat[:, piece * LANES:(piece + 1) * LANES]
                if block < 2:
                    place = block * 512 + piece * LANES
                    qs[:, place:place + LANES] = (rotated(values) * head ** -0.5).astype(BF16)
                elif block == 2:
                    doubled(rotated(values), ks, piece)
                else:
                    doubled(values, vs, piece)

        chunk = 256
        chunk_low = lax.broadcasted_iota(jnp.int32, (chunk, LANES), 1) < head
        inside = lax.rem(lax.broadcasted_iota(jnp.int32, (2 * chunk, chunk), 0), chunk) >= lax.broadcasted_iota(jnp.int32, (2 * chunk, chunk), 1)

        def columns(index):
            return pl.ds(pl.multiple_of(index * LANES, LANES), LANES)

        def score(index, parts, target):
            cols, place = columns(index), 0
            for part in parts:
                span = (part + 1) * chunk
                q_part = qs[part * chunk:span, cols]
                none = jnp.zeros_like(q_part)
                pair = jnp.concatenate([jnp.where(chunk_low, q_part, none), jnp.where(chunk_low, none, q_part)], axis=0)
                scores = matmul_t(pair, ks[:span, cols])
                edge = jnp.where(inside, scores[:, part * chunk:], -1e30)
                scores = edge if part == 0 else jnp.concatenate([scores[:, :part * chunk], edge], axis=1)
                target[:, place:place + span] = scores
                tops[part] = jnp.broadcast_to(jnp.max(scores, axis=1, keepdims=True), tops.shape[1:])
                place += span

        def soften(parts, origin, target):
            place = 0
            for part in parts:
                top = tops[part]
                total = jnp.zeros_like(top)
                for _ in range((part + 1) * chunk // LANES):
                    powers = jnp.exp(origin[:, place:place + LANES] - top)
                    total = total + powers
                    target[:, place:place + LANES] = powers.astype(BF16)
                    place += LANES
                sums[part] = jnp.broadcast_to(jnp.sum(total, axis=1, keepdims=True), sums.shape[1:])

        def mix(index, parts, origin):
            cols, place = columns(index), 0
            for part in parts:
                span = (part + 1) * chunk
                mixed = matmul(origin[:, place:place + span], vs[:span, cols]) / sums[part]
                os[part * chunk:span, cols] = jnp.where(chunk_low, mixed[:chunk], mixed[chunk:]).astype(BF16)
                place += span

        outer_parts, inner_parts = (0, 3), (1, 2)
        score(0, outer_parts, s_outer)

        def group(index, inner):
            score(index, inner_parts, s_inner)
            soften(outer_parts, s_outer, p_outer)
            mix(lax.rem(index + kv_heads - 1, kv_heads), inner_parts, p_inner)
            score(lax.rem(index + 1, kv_heads), outer_parts, s_outer)
            soften(inner_parts, s_inner, p_inner)
            mix(index, outer_parts, p_outer)
            return inner

        lax.fori_loop(0, kv_heads, group, 0)
        mix(kv_heads - 1, inner_parts, p_inner)

        def project(index, inner):
            local = pl.ds(pl.multiple_of(index * tile, tile), tile)
            part = pl.ds(pl.multiple_of(base + index * tile, tile), tile)
            added = matmul(os[local, :tile], wo[0]) + matmul(os[local, tile:], wo[1])
            after = (acc[part, :] + added).astype(BF16).astype(F32)
            acc[part, :] = after
            xs[0, part, :] = (after * norm_scale_of(after) * norm_ffn).astype(BF16)
            return inner

        lax.fori_loop(0, seq // tile, project, 0)
        return carry

    lax.fori_loop(0, micro, sequence, 0)

    big = 1024
    lanes = lax.broadcasted_iota(jnp.int32, (big, LANES), 1)
    moments = {5: 2, 14: 3, 21: 4, 24: 5}

    def ffn_step(dense, step, carry):
        slot = lax.rem(step, 2)
        for copy in expert_copies(slot, (gg_hbm.at[0], gu_hbm.at[0], gd_hbm.at[0])):
            copy.wait()
        for moment, point in moments.items():
            if dense == (moment < ffn_steps):
                @pl.when(step == moment)
                def _():
                    service(point)

        prefetch(step + 1, 1 - slot)
        gate_w, up_w, down_w = wg.at[slot], wu.at[slot], wd.at[slot]

        def rows_step(index, inner):
            part = pl.ds(pl.multiple_of(index * big, big), big)
            tokens = xs[0 if dense else 1, part, :]
            mixed = jax.nn.silu(matmul(tokens, gate_w[...])) * matmul(tokens, up_w[...])
            if dense:
                acc[part, :] += matmul(mixed.astype(BF16), down_w[...])
            else:
                weight = jnp.sum(jnp.where(lanes == step - ffn_steps, gates[part, :], 0.0), axis=1, keepdims=True)
                mixed = jnp.where(weight > 0.0, mixed, 0.0).astype(BF16)
                acc[part, :] += weight * matmul(mixed, down_w[...]).astype(BF16).astype(F32)
            return inner

        if dense:
            lax.fori_loop(0, rows // big, rows_step, 0)
        else:
            for index in range(rows // big):
                rows_step(index, 0)
        return carry

    lax.fori_loop(0, ffn_steps, functools.partial(ffn_step, True), 0)
    lax.fori_loop(ffn_steps, steps, functools.partial(ffn_step, False), 0)

    results[-1].start()
    service(len(waits) - 1)
    for block in range(STATIC // 2, len(BLOCKS)):
        d2d_wait(block, pieces_of(block))
    for stage in plan:
        for entry in stage:
            ici_copy(*entry).wait_send()
    for block in range(len(BLOCKS)):
        for piece in pieces_of(block):
            d2d_copy(block, piece, piece_ref(block, piece)).wait_send()
    for copy in results:
        copy.wait()


def compact_kernel(
    dims,
    picks_hbm, shares_hbm, counts_hbm, tokens_hbm, base_hbm, gg_hbm, gu_hbm, gd_hbm,
    out_hbm,
    picks, shares, counts, tokens, base, table, total, packed, lhs, result, wg, wu, wd,
    load_sem, w_sem, out_sem,
):
    rows, width, first, ranks = dims
    list_size = rows // 2 + TILE
    parts = width // LANES
    experts = first + ranks
    loads = [pltpu.make_async_copy(source, target, load_sem.at[k]) for k, (source, target) in enumerate((
        (tokens_hbm, tokens), (picks_hbm, picks), (shares_hbm, shares), (counts_hbm, counts), (base_hbm, base)))]
    for copy in loads:
        copy.start()

    def weights(rank, slot):
        return [pltpu.make_async_copy(source.at[first + rank], buffer.at[slot], w_sem.at[slot, k])
                for k, (source, buffer) in enumerate(((gg_hbm, wg), (gu_hbm, wu), (gd_hbm, wd)))]

    for copy in weights(0, 0):
        copy.start()

    loads[0].wait()
    table[0] = jnp.zeros((parts, LANES), F32)
    total[0] = jnp.zeros((parts, LANES), F32)
    flat = table.reshape((rows + 1) * parts, LANES)
    step_rows = 512

    def spread(index, carry):
        start = pl.multiple_of(index * step_rows, step_rows)
        values = tokens[pl.ds(start, step_rows), :].astype(F32)
        for part in range(parts):
            flat[pl.ds(parts + start * parts + part, step_rows, stride=parts), :] = values[:, part * LANES:(part + 1) * LANES]
        total[pl.ds(1 + start, step_rows)] = jnp.zeros((step_rows, parts, LANES), F32)
        return carry

    lax.fori_loop(0, rows // step_rows, spread, 0)
    for copy in loads[1:4]:
        copy.wait()

    def tiles_of(rank):
        return jnp.maximum((counts[0, first + rank] + TILE - 1) // TILE, 1)

    def gather(rank, tile):
        start = rank * list_size + tile * TILE
        for place in range(TILE):
            packed[place] = table[picks[start + place]]

    def scatter(rank, tile):
        start = rank * list_size + tile * TILE
        for group in range(0, TILE, UNIT):
            rows_of = [picks[start + group + place] for place in range(UNIT)]
            sums = [total[row] + result.reshape(TILE * parts, LANES)[pl.ds(group * parts + place, parts, stride=UNIT), :] for place, row in enumerate(rows_of)]
            for row, value in zip(rows_of, sums):
                total[row] = value

    def factor(rank, tile):
        line = (rank * list_size + tile * TILE) // LANES
        lines = [jnp.broadcast_to(shares[pl.ds(line + k, 1), :], (LANES, LANES)).T for k in range(TILE // LANES)]
        return jnp.concatenate(lines, axis=0)

    count = lax.fori_loop(0, ranks, lambda rank, so_far: so_far + tiles_of(rank), 0)
    gather(0, 0)

    def tile_step(index, carry):
        rank, tile, last_rank, last_tile = carry
        slot = lax.rem(rank, 2)

        @pl.when(tile == 0)
        def _():
            for copy in weights(rank, slot):
                copy.wait()

            @pl.when(rank + 1 < ranks)
            def _():
                for copy in weights(rank + 1, 1 - slot):
                    copy.start()

        more = tile + 1 < tiles_of(rank)
        next_rank = jnp.where(more, rank, rank + 1)
        next_tile = jnp.where(more, tile + 1, 0)
        for part in range(parts):
            lhs[:, part * LANES:(part + 1) * LANES] = packed.reshape(TILE * parts, LANES)[pl.ds(part, TILE, stride=parts), :].astype(BF16)
        scatter(last_rank, last_tile)
        gather(next_rank, next_tile)
        gate_act = matmul(lhs[...], wg[slot])
        up_act = matmul(lhs[...], wu[slot])
        mixed = (jax.nn.silu(gate_act) * up_act).astype(BF16)
        down = matmul(mixed, wd[slot]).astype(BF16).astype(F32)
        share = factor(rank, tile)
        for part in range(parts):
            result[:, part] = (share * down[:, part * LANES:(part + 1) * LANES]).reshape(TILE // UNIT, UNIT, LANES)
        return next_rank, next_tile, rank, tile

    _, _, last_rank, last_tile = lax.fori_loop(0, count, tile_step, (jnp.int32(0), jnp.int32(0), jnp.int32(ranks), jnp.int32(0)))
    scatter(last_rank, last_tile)
    loads[4].wait()
    sums_of = total.reshape((rows + 1) * parts, LANES)

    def store(index):
        part = pl.ds(index * step_rows, step_rows)
        return pltpu.make_async_copy(tokens.at[part], out_hbm.at[part], out_sem.at[index])

    def finish(index, carry):
        start = pl.multiple_of(index * LANES, LANES)
        for part in range(parts):
            cols = slice(part * LANES, (part + 1) * LANES)
            moe = sums_of[pl.ds(parts + start * parts + part, LANES, stride=parts), :]
            tokens[pl.ds(start, LANES), cols] = (base[pl.ds(start, LANES), cols] + moe).astype(BF16)
        return carry

    for index in range(rows // step_rows):
        lax.fori_loop(index * step_rows // LANES, (index + 1) * step_rows // LANES, finish, 0)
        store(index).start()
    for index in range(rows // step_rows):
        store(index).wait()

def rope_tables(seq, head):
    half = head // 2
    freqs = np.float32(ROPE_BASE) ** (-np.arange(half, dtype=np.float32) * np.float32(2.0) / np.float32(head))
    angles = np.arange(seq, dtype=np.float32)[:, None] * freqs.astype(np.float32)[None, :]
    cosine = np.cos(angles.astype(np.float64)).astype(np.float32)
    sine = np.sin(angles.astype(np.float64)).astype(np.float32)
    times = LANES // head
    return np.stack([np.tile(np.concatenate([cosine, cosine], 1), (1, times)), np.tile(np.concatenate([-sine, sine], 1), (1, times))])


def solution(mesh):
    tok_spec = P(None, ('dp', 'ep'), None, None)
    rep_one = P(None)
    rep_two = P(None, None)
    rep_three = P(None, None, None)
    expert_spec = P('ep', None, None)
    assert mesh.shape['ep'] == 2 * SIDE * SIDE

    def local_program(resid_in, expert_idx, expert_slot, w_query, w_key, w_value, w_out, w_gate, w_up, w_down, w_router, norm_attn, norm_ffn, norm_moe, expert_gate, expert_up, expert_down):
        micro, seqs, seq, width = resid_in.shape
        choices = expert_idx.shape[-1]
        heads, head = w_query.shape[1:]
        kv_heads = w_key.shape[1]
        hidden = expert_gate.shape[2]
        experts = 2 * len(BLOCKS)
        rows = micro * seqs * seq
        ids = expert_idx.transpose(0, 1, 3, 2).reshape(micro * seqs, choices, seq)
        rope = jnp.asarray(rope_tables(seq, head))
        anywhere = pl.BlockSpec(memory_space=pl.ANY)
        operands = (
            resid_in.reshape(rows, width), ids, w_router.T, norm_attn, norm_ffn, norm_moe, rope,
            w_query.transpose(1, 2, 0).reshape(heads * head, width), w_key.transpose(1, 2, 0).reshape(kv_heads * head, width),
            w_value.transpose(1, 2, 0).reshape(kv_heads * head, width), w_out.reshape(heads * head, width),
            w_gate, w_up, w_down, expert_gate, expert_up, expert_down)
        flops = rows * width * 2 * (3 * hidden * experts + 3 * w_gate.shape[1] + 3 * heads * head)
        late = experts - STATIC
        list_size = rows // 2 + TILE
        lists = ((late + 1) * list_size // LANES, LANES)
        weight_shapes = ((width, hidden), (width, hidden), (hidden, width))
        double = [pltpu.VMEM((2,) + shape, BF16) for shape in weight_shapes]
        base, tokens, picks, shares, counts, gate_all, up_all, down_all = pl.pallas_call(
            functools.partial(fused_kernel, (rows, width, seq, hidden, heads, kv_heads, head)),
            out_shape=tuple(jax.ShapeDtypeStruct(shape, kind) for shape, kind in (
                ((rows, width), F32), ((rows, width), BF16), (lists, jnp.int32), (lists, F32), ((UNIT, LANES), jnp.int32),
                *[((experts,) + shape, BF16) for shape in weight_shapes])),
            in_specs=[anywhere] * len(operands),
            out_specs=[anywhere] * 8,
            scratch_shapes=[
                pltpu.VMEM(lists, jnp.int32),
                pltpu.VMEM(lists, F32),
                pltpu.VMEM((experts, 512), F32),
                pltpu.VMEM((UNIT, LANES), jnp.int32),
                pltpu.VMEM((2, rows, width), BF16),
                pltpu.VMEM((rows, width), F32),
                pltpu.VMEM((rows, LANES), F32),
                *[pltpu.VMEM((seq, heads * head), BF16) for _ in range(4)],
                *[pltpu.VMEM((512, 1280), kind) for kind in (F32, F32, BF16, BF16)],
                *[pltpu.VMEM((4, 512, LANES), F32) for _ in range(2)],
                pltpu.VMEM((micro * seqs, choices, seq), jnp.int32),
                pltpu.VMEM((experts, width), BF16),
                *[pltpu.VMEM((width,), BF16) for _ in range(3)],
                pltpu.VMEM((2, seq, LANES), F32),
                pltpu.VMEM((4, 512, width), BF16),
                pltpu.VMEM((2, 512, width), BF16),
                *double,
                *[pltpu.SemaphoreType.DMA(shape) for shape in ((13,), (2, 3), (5,), (4, 16), (16, 8), (16, 8), (16, 8))],
            ],
            compiler_params=pltpu.CompilerParams(collective_id=0, has_side_effects=True, vmem_limit_bytes=62 * 1024 * 1024),
            cost_estimate=pl.CostEstimate(flops=flops, bytes_accessed=experts * 6 * width * hidden, transcendentals=0),
        )(*operands)
        parts = width // LANES
        picks = picks.reshape(-1)
        staged = pltpu.VMEM((TILE // UNIT, parts, UNIT, LANES), F32)
        out = pl.pallas_call(
            functools.partial(compact_kernel, (rows, width, STATIC, late)),
            out_shape=jax.ShapeDtypeStruct((rows, width), BF16),
            in_specs=[anywhere] * 8,
            out_specs=anywhere,
            scratch_shapes=[
                pltpu.SMEM((picks.size,), jnp.int32),
                pltpu.VMEM(lists, F32),
                pltpu.SMEM((UNIT, LANES), jnp.int32),
                pltpu.VMEM((rows, width), BF16),
                pltpu.VMEM((rows, width), F32),
                *[pltpu.VMEM((rows + 1, parts, LANES), F32) for _ in range(2)],
                pltpu.VMEM((TILE, parts, LANES), F32),
                pltpu.VMEM((TILE, width), BF16),
                staged,
                *double,
                *[pltpu.SemaphoreType.DMA(shape) for shape in ((5,), (2, 3), (4,))],
            ],
            compiler_params=pltpu.CompilerParams(vmem_limit_bytes=62 * 1024 * 1024),
        )(picks, shares, counts, tokens, base, gate_all, up_all, down_all)
        return out.reshape(resid_in.shape)

    return jax.shard_map(local_program, mesh=mesh, in_specs=(tok_spec, tok_spec, tok_spec, rep_three, rep_three, rep_three, rep_three, rep_two, rep_two, rep_two, rep_two, rep_one, rep_one, rep_one, expert_spec, expert_spec, expert_spec), out_specs=tok_spec, check_vma=False)
```
